512 devices in a mesh: seq: 32 (over z_hi, y, core), mp: 16 (over z_lo, x).
Axes of the slice: x: 4, y: 8, z: 8 (z_hi: 2, z_lo: 4; z = z_hi * 4 + z_lo), core: 2. Of those that a mesh axis runs over, the one named last changes fastest.
Arguments:
- inputs: bfloat16 [32768, 4096], P('seq', 'mp'), may hold values from -6 to 6
- conv_weight: bfloat16 [4, 4096], P(None, 'mp'), may hold values from -3 to 3
- conv_bias: bfloat16 [4096], P('mp'), may hold values from -3 to 3
- doc_start: int32 [32768], P('seq'), may hold values from 0 to 32767, as said below
- counts: int32 [32], P('seq'), may hold values from 341 to 1024
Outputs:
- gram: float32 [4096, 4096], P('seq', 'mp')
The draws below stay inside these ranges and needn't reach their ends.
Inputs may be any that keep to these rules, and one draw needn't show every extreme that they name: doc_start is never above the token's own position, and for t > 0 either doc_start[t] == t or doc_start[t] == doc_start[t - 1]; doc_start[0] is 0.
All inputs are finite; a program needn't handle non-finite values.
Results may differ from the reference program's by a relative error of at most 0.0003.
Values may be sent and summed in bfloat16 or wider, within the bound.
No kernel may reach another device: no remote copies, remote signals or barrier semaphores. Data moves between devices by JAX's collectives and lax.ppermute only.
A program may use at most 64 MiB of HBM per device.

```python
import jax
import jax.numpy as jnp
from jax import lax

C = 4096
KERNEL = 4
TOK_DEV = 1024
TOKENS = 32768
SHARDS = 32


def draw_doc_start(key, part):
    flags = jax.random.randint(key, (TOKENS,), 0, max(TOK_DEV // 4, 2)) == 0
    flags = flags.at[0].set(True).at[TOKENS - 1].set(True)
    position = jnp.arange(TOKENS, dtype=jnp.int32)
    starts = jnp.where(flags, position, 0)
    return lax.cummax(starts, axis=0).astype(jnp.int32)


def draw_counts(key, part):
    shard_ids = jnp.arange(SHARDS, dtype=jnp.int32)
    spread = TOK_DEV - TOK_DEV // 3 - TOK_DEV // 8
    base = TOK_DEV // 3 + shard_ids * spread // (SHARDS - 1)
    jitter = jax.random.randint(key, (SHARDS,), 0, TOK_DEV // 8 + 1)
    values = jnp.minimum(base + jitter, TOK_DEV)
    return values.at[SHARDS - 1].set(TOK_DEV).astype(jnp.int32)


def block_scale(key, dims, pieces, low, top_value):
    loudness, own = 1.0, jax.random.fold_in(key, 6)
    for axis_at, blocks in pieces:
        draws = jnp.exp(jax.random.uniform(jax.random.fold_in(own, axis_at), (blocks,), jnp.float32, low / len(pieces), top_value / len(pieces)))
        loudness = loudness * jnp.repeat(draws, dims[axis_at] // blocks).reshape([-1 if axis == axis_at else 1 for axis in range(len(dims))])
    return loudness


def gaussian(stream_key, extent, scale, most, split=(), kind=jnp.bfloat16):
    entries = jax.random.normal(stream_key, extent, jnp.float32) * scale
    if len(split) > 0:
        entries = block_scale(stream_key, extent, split, -0.22, 0.18) * entries
    return jnp.clip(entries, min=-most, max=most).astype(kind)


def setup_inputs(seed: int = 0) -> dict:
    seeds = jax.random.split(jax.random.key(seed), 6)
    return {
        "inputs": gaussian(seeds[0], (TOKENS, C), 1.0, 6.0, ((0, 32), (1, 16))),
        "conv_weight": gaussian(seeds[1], (KERNEL, C), KERNEL ** -0.5, 3.0, ((1, 16),)),
        "conv_bias": gaussian(seeds[2], (C,), 0.5, 3.0, ((0, 16),)),
        "doc_start": draw_doc_start(jax.random.fold_in(seeds[5], 71), 0),
        "counts": draw_counts(jax.random.fold_in(seeds[5], 71), 0),
    }


def causal_conv(extended, weights, bias, position, doc_start, length):
    kernel_len = weights.shape[0]
    summed = jnp.zeros((length, weights.shape[1]), jnp.float32) + bias.astype(jnp.float32)
    for lag in range(kernel_len):
        window = extended[kernel_len - 1 - lag: kernel_len - 1 - lag + length].astype(jnp.float32)
        usable = (position - lag) >= doc_start
        summed = summed + jnp.where(usable[:, None], weights[lag].astype(jnp.float32) * window, 0.0)
    return jax.nn.silu(summed).astype(jnp.bfloat16)


def reference(inputs, conv_weight, conv_bias, doc_start, counts):
    position = jnp.arange(TOKENS, dtype=jnp.int32)
    padding = jnp.zeros((KERNEL - 1, C), jnp.bfloat16)
    extended = jnp.concatenate([padding, inputs], axis=0)
    feats = causal_conv(extended, conv_weight, conv_bias, position, doc_start, TOKENS)
    counted = (position % TOK_DEV) < jnp.repeat(counts, TOK_DEV)
    kept = jnp.where(counted[:, None], feats, jnp.zeros_like(feats))

    def add_block(carry, pair):
        left, right = pair
        return carry + lax.dot_general(left, right, (((0,), (0,)), ((), ())), preferred_element_type=jnp.float32), None

    summed, _ = lax.scan(add_block, jnp.zeros((C, C), jnp.float32),
                         (feats.reshape(SHARDS, TOK_DEV, C), kept.reshape(SHARDS, TOK_DEV, C)))
    token_total = jnp.sum(counts.astype(jnp.float32))
    return summed / token_total
```

```python
import jax
import jax.numpy as jnp
import numpy as np
from jax import lax
from jax.experimental import pallas as pl
from jax.experimental.pallas import tpu as pltpu
from jax.sharding import Mesh
from jax.sharding import PartitionSpec as P

ZH, YW, YA, CORE, ZL, X = AXES = ("zh", "yw", "ya", "core", "zl", "x")
SIZES = (2, 2, 4, 2, 4, 4)
SEQ = (ZH, YW, YA, CORE)
Y = (YW, YA)
CHIPS = (ZH, YW, YA)
TAU = (2, 3, 1, 0)
HALF = 128


def delivery():
    def number(seq_chip, core, mp):
        return (seq_chip * 2 + core) * 16 + mp

    edges = []
    for seq_chip in range(16):
        for h in range(2):
            for mp in range(16):
                zeta, a = divmod(seq_chip, 4)
                z, x = divmod(mp, 4)
                row = 4 * z + a
                if zeta == z:
                    col, hc = 4 * z + x, (h if a >= x else 1 - h)
                elif zeta == z ^ 1:
                    col, hc = 4 * (z ^ 1) + x, (h if z % 2 else 1 - h)
                else:
                    col, hc = 4 * TAU[z] + x, (0 if zeta == z ^ 2 else 1)
                src = number(seq_chip, h, mp)
                if row == col:
                    continue
                edges.append((src, number(row, h, col), hc, 0))
                edges.append((src, number(col, hc, row), h, 1))
    by_src, by_dst = {}, {}
    for e, (s, d, _, _) in enumerate(edges):
        by_src.setdefault(s, []).append(e)
        by_dst.setdefault(d, []).append(e)
    colour = {}
    for first in range(len(edges)):
        e = first
        while e not in colour:
            colour[e] = 0
            s = edges[e][0]
            other = [k for k in by_src[s] if k != e][0]
            colour[other] = 1
            d = edges[other][1]
            e = [k for k in by_dst[d] if k != other][0]
    pairs = ([], [])
    table = np.zeros((512, 4), np.int32)
    for e, (s, d, half, turned) in enumerate(edges):
        k = colour[e]
        pairs[k].append((s, d))
        table[d, 2 * k] = turned
        table[d, 2 * k + 1] = half
    for mp in range(16):
        for h in range(2):
            own, other = number(mp, h, mp), number(mp, 1 - h, mp)
            pairs[1].append((own, other))
            table[own] = (0, h, h, 1 - h)
    return pairs, table


def around(x, axis, by):
    n = lax.axis_size(axis)
    return lax.ppermute(x, axis, [((i + by) % n, i) for i in range(n)])


def flipped(x, axis):
    n = lax.axis_size(axis)
    return lax.ppermute(x, axis, [(i, i ^ 1) for i in range(n)])


def products(where_ref, f0, f1, f2, f3, c1, ct, keep, send):
    x, z, core = where_ref[0], where_ref[1], where_ref[2]
    dims = (((0,), (0,)), ((), ()))
    for o, f in enumerate((f0, f1, f2, f3)):
        a = lax.rem(x + o, 4)

        def put(zeta, q0, q1):
            slot = zeta * 4 + a
            keep[slot] = jnp.where(core == 0, q0, q1)
            send[slot] = jnp.where(core == 0, q1, q0)

        lhs = f[...]
        for k, c in enumerate((f0, c1, ct)):
            p = lax.dot_general(lhs, c[...], dims, preferred_element_type=jnp.float32)
            p00, p01, p10, p11 = p[:HALF, :HALF], p[:HALF, HALF:], p[HALF:, :HALF], p[HALF:, HALF:]
            if k < 2:
                same = (a >= x) if k == 0 else (lax.rem(z, 2) == 1)
                put(z if k == 0 else z ^ 1, jnp.where(same, p00, p01), jnp.where(same, p11, p10))
            else:
                put(z ^ 2, p00, p10)
                put(z ^ 3, p01, p11)


def all_products(where, rows, c1, ct):
    shape = jax.ShapeDtypeStruct((16, HALF, HALF), jnp.float32)
    vmem = pl.BlockSpec(memory_space=pltpu.VMEM)
    return pl.pallas_call(
        products,
        out_shape=(shape, shape),
        in_specs=[pl.BlockSpec(memory_space=pltpu.SMEM)] + [vmem] * 6,
        out_specs=(vmem, vmem),
        compiler_params=pltpu.CompilerParams(vmem_limit_bytes=16 << 20),
        cost_estimate=pl.CostEstimate(flops=2 * 1024 * 1024 * 768, bytes_accessed=5 << 20, transcendentals=0),
        name="products",
    )(where, *rows, c1, ct)


def causal_conv(extended, weights, bias, position, doc_start, counted, length):
    taps = weights.shape[0]
    summed = jnp.zeros((length, weights.shape[1]), jnp.float32) + bias.astype(jnp.float32)
    for lag in range(taps):
        window = extended[taps - 1 - lag : taps - 1 - lag + length].astype(jnp.float32)
        usable = position - lag >= doc_start
        summed = summed + jnp.where(usable[:, None], weights[lag].astype(jnp.float32) * window, 0.0)
    return jnp.where(counted[:, None], jax.nn.silu(summed), 0.0).astype(jnp.bfloat16)


def on_device(inputs, conv_weight, conv_bias, doc_start, counts):
    pairs, table = delivery()
    length, width = inputs.shape
    taps = conv_weight.shape[0]
    core, z, x = lax.axis_index(CORE), lax.axis_index(ZL), lax.axis_index(X)
    chip = lax.axis_index(CHIPS)

    count = counts[0]
    tail = jnp.concatenate(
        [
            inputs[length - (taps - 1) :],
            jnp.full((1, width), (count // 32).astype(jnp.bfloat16)),
            jnp.full((1, width), (count % 32).astype(jnp.bfloat16)),
        ],
        axis=0,
    )
    shards = lax.axis_size(SEQ)
    prior = lax.ppermute(tail, SEQ, [(i, (i + 1) % shards) for i in range(shards)])
    count_pair = (
        count.astype(jnp.float32)
        + prior[taps - 1, 0].astype(jnp.float32) * 32.0
        + prior[taps, 0].astype(jnp.float32)
    )
    position = lax.axis_index(SEQ) * length + jnp.arange(length, dtype=jnp.int32)
    counted = jnp.arange(length, dtype=jnp.int32) < count
    extended = jnp.concatenate([prior[: taps - 1], inputs], axis=0)
    own = causal_conv(extended, conv_weight, conv_bias, position, doc_start, counted, length)

    c1 = flipped(own, ZL)
    f1 = around(own, X, 1)
    f3 = around(own, X, 3)
    ct = lax.ppermute(own, ZL, [(TAU[i], i) for i in range(4)])
    f2 = around(own, X, 2)

    corner = lax.dot_general(
        own[:, :HALF], own[:, HALF:], (((0,), (0,)), ((), ())), preferred_element_type=jnp.float32
    )
    goal = lax.rem(z, 2) * 4 + x
    pieces = jnp.where((jnp.arange(8, dtype=jnp.int32) == goal)[:, None, None], corner[None], 0.0)
    pieces = jnp.concatenate([pieces, jnp.full((8, 8, HALF), count_pair)], axis=1)
    early = lax.all_to_all(pieces, Y, split_axis=0, concat_axis=0, tiled=True).sum(axis=0)
    early = early + flipped(early, ZH)
    corner, total = early[:HALF], early[HALF, 0]

    where = jnp.stack([x, z, core]).astype(jnp.int32)
    keep, send = all_products(where, (own, f1, f2, f3), c1, ct)
    mine = keep + flipped(send, CORE)
    quad = lax.all_to_all(mine, CHIPS, split_axis=0, concat_axis=0, tiled=True).sum(axis=0)

    diagonal = chip == 4 * z + x
    r1 = lax.ppermute(quad, AXES, pairs[0])
    r2 = lax.ppermute(jnp.where(diagonal, corner, quad), AXES, pairs[1])
    me = jnp.asarray(table)[lax.axis_index(AXES)]
    r1 = jnp.where(diagonal, quad, r1)
    r2 = jnp.where(diagonal, corner + r2, r2)
    r1 = jnp.where(me[0] == 1, r1.T, r1)
    r2 = jnp.where(me[2] == 1, r2.T, r2)
    first = me[1] == 0
    summed = jnp.concatenate([jnp.where(first, r1, r2), jnp.where(first, r2, r1)], axis=1)
    return summed / total


def solution(mesh):
    torus = Mesh(mesh.devices.reshape(SIZES), AXES)
    mp = (ZL, X)
    placed = (P(SEQ, mp), P(None, mp), P(mp), P(SEQ), P(SEQ))
    return jax.shard_map(on_device, mesh=torus, in_specs=placed, out_specs=P(SEQ, mp), check_vma=False)
```

```python
import jax
import jax.numpy as jnp
import numpy as np
from jax import lax
from jax.experimental import pallas as pl
from jax.experimental.pallas import tpu as pltpu
from jax.sharding import Mesh
from jax.sharding import PartitionSpec as P


ZH, YW, YA, CORE, ZL, X = AXES = ("zh", "yw", "ya", "core", "zl", "x")
SIZES = (2, 2, 4, 2, 4, 4)
SEQ = (ZH, YW, YA, CORE)
Y = (YW, YA)
CHIPS = (ZH, YW, YA)
TAU = (2, 3, 1, 0)
HALF = 128


def delivery():
    def number(seq_chip, core, mp):
        return (seq_chip * 2 + core) * 16 + mp

    edges = []
    for seq_chip in range(16):
        for h in range(2):
            for mp in range(16):
                zeta, a = divmod(seq_chip, 4)
                z, x = divmod(mp, 4)
                row = 4 * z + a
                if zeta == z:
                    col, hc = 4 * z + x, (h if a >= x else 1 - h)
                elif zeta == z ^ 1:
                    col, hc = 4 * (z ^ 1) + x, (h if z % 2 else 1 - h)
                else:
                    col, hc = 4 * TAU[z] + x, (0 if zeta == z ^ 2 else 1)
                src = number(seq_chip, h, mp)
                if row == col:
                    continue
                edges.append((src, number(row, h, col), hc, 0))
                edges.append((src, number(col, hc, row), h, 1))
    by_src, by_dst = {}, {}
    for e, (s, d, _, _) in enumerate(edges):
        by_src.setdefault(s, []).append(e)
        by_dst.setdefault(d, []).append(e)
    colour = {}
    for first in range(len(edges)):
        e = first
        while e not in colour:
            colour[e] = 0
            s = edges[e][0]
            other = [k for k in by_src[s] if k != e][0]
            colour[other] = 1
            d = edges[other][1]
            e = [k for k in by_dst[d] if k != other][0]
    pairs = ([], [])
    table = np.zeros((512, 4), np.int32)
    for e, (s, d, half, turned) in enumerate(edges):
        k = colour[e]
        pairs[k].append((s, d))
        table[d, 2 * k] = turned
        table[d, 2 * k + 1] = half
    for mp in range(16):
        for h in range(2):
            own, other = number(mp, h, mp), number(mp, 1 - h, mp)
            pairs[1].append((own, other))
            table[own] = (0, h, h, 1 - h)
    return pairs, table


def around(x, axis, by):
    n = lax.axis_size(axis)
    return lax.ppermute(x, axis, [((i + by) % n, i) for i in range(n)])


def flipped(x, axis):
    n = lax.axis_size(axis)
    return lax.ppermute(x, axis, [(i, i ^ 1) for i in range(n)])


def products(where_ref, f0, f1, f2, f3, c1, ct, keep, send):
    x, z, core = where_ref[0], where_ref[1], where_ref[2]
    dims = (((0,), (0,)), ((), ()))
    for o, f in enumerate((f0, f1, f2, f3)):
        a = lax.rem(x + o, 4)

        def put(zeta, q0, q1):
            slot = zeta * 4 + a
            keep[slot] = jnp.where(core == 0, q0, q1)
            send[slot] = jnp.where(core == 0, q1, q0)

        lhs = f[...]
        for k, c in enumerate((f0, c1, ct)):
            p = lax.dot_general(lhs, c[...], dims, preferred_element_type=jnp.float32)
            p00, p01, p10, p11 = p[:HALF, :HALF], p[:HALF, HALF:], p[HALF:, :HALF], p[HALF:, HALF:]
            if k < 2:
                same = (a >= x) if k == 0 else (lax.rem(z, 2) == 1)
                put(z if k == 0 else z ^ 1, jnp.where(same, p00, p01), jnp.where(same, p11, p10))
            else:
                put(z ^ 2, p00, p10)
                put(z ^ 3, p01, p11)


def all_products(where, rows, c1, ct):
    shape = jax.ShapeDtypeStruct((16, HALF, HALF), jnp.float32)
    vmem = pl.BlockSpec(memory_space=pltpu.VMEM)
    return pl.pallas_call(
        products,
        out_shape=(shape, shape),
        in_specs=[pl.BlockSpec(memory_space=pltpu.SMEM)] + [vmem] * 6,
        out_specs=(vmem, vmem),
        compiler_params=pltpu.CompilerParams(vmem_limit_bytes=16 << 20),
        cost_estimate=pl.CostEstimate(flops=2 * 1024 * 1024 * 768, bytes_accessed=5 << 20, transcendentals=0),
        name="products",
    )(where, *rows, c1, ct)


def causal_conv(extended, weights, bias, position, doc_start, counted, length):
    taps = weights.shape[0]
    summed = jnp.zeros((length, weights.shape[1]), jnp.float32) + bias.astype(jnp.float32)
    for lag in range(taps):
        window = extended[taps - 1 - lag : taps - 1 - lag + length].astype(jnp.float32)
        usable = position - lag >= doc_start
        summed = summed + jnp.where(usable[:, None], weights[lag].astype(jnp.float32) * window, 0.0)
    return jnp.where(counted[:, None], jax.nn.silu(summed), 0.0).astype(jnp.bfloat16)


def on_device(inputs, conv_weight, conv_bias, doc_start, counts):
    pairs, table = delivery()
    length, width = inputs.shape
    taps = conv_weight.shape[0]
    core, z, x = lax.axis_index(CORE), lax.axis_index(ZL), lax.axis_index(X)
    chip = lax.axis_index(CHIPS)

    count = counts[0]
    tail = jnp.concatenate(
        [
            inputs[length - (taps - 1) :],
            jnp.full((1, width), (count // 32).astype(jnp.bfloat16)),
            jnp.full((1, width), (count % 32).astype(jnp.bfloat16)),
        ],
        axis=0,
    )
    shards = lax.axis_size(SEQ)
    prior = lax.ppermute(tail, SEQ, [(i, (i + 1) % shards) for i in range(shards)])
    count_pair = (
        count.astype(jnp.float32)
        + prior[taps - 1, 0].astype(jnp.float32) * 32.0
        + prior[taps, 0].astype(jnp.float32)
    )
    position = lax.axis_index(SEQ) * length + jnp.arange(length, dtype=jnp.int32)
    counted = jnp.arange(length, dtype=jnp.int32) < count
    extended = jnp.concatenate([prior[: taps - 1], inputs], axis=0)
    own = causal_conv(extended, conv_weight, conv_bias, position, doc_start, counted, length)

    ct = lax.ppermute(own, ZL, [(TAU[i], i) for i in range(4)])
    f1 = around(own, X, 1)
    f3 = around(own, X, 3)
    c1 = flipped(own, ZL)
    f2 = around(own, X, 2)

    corner = lax.dot_general(
        own[:, :HALF], own[:, HALF:], (((0,), (0,)), ((), ())), preferred_element_type=jnp.float32
    )
    goal = lax.rem(z, 2) * 4 + x
    pieces = jnp.where((jnp.arange(8, dtype=jnp.int32) == goal)[:, None, None], corner[None], 0.0)
    pieces = jnp.concatenate([pieces, jnp.full((8, 8, HALF), count_pair)], axis=1)
    early = lax.all_to_all(pieces, Y, split_axis=0, concat_axis=0, tiled=True)
    early = early.sum(axis=0)
    early = early + flipped(early, ZH)
    corner, total = early[:HALF], early[HALF, 0]

    where = jnp.stack([x, z, core]).astype(jnp.int32)
    f1, f2, f3, c1, ct, corner, total = lax.optimization_barrier((f1, f2, f3, c1, ct, corner, total))
    keep, send = all_products(where, (own, f1, f2, f3), c1, ct)
    mine = keep + flipped(send, CORE)
    quad = lax.all_to_all(mine, CHIPS, split_axis=0, concat_axis=0, tiled=True).sum(axis=0)

    diagonal = chip == 4 * z + x
    second = lax.optimization_barrier(jnp.where(diagonal, corner, quad))
    r1 = lax.ppermute(quad, AXES, pairs[0])
    r2 = lax.ppermute(second, AXES, pairs[1])
    r1, r2 = lax.optimization_barrier((r1, r2))
    me = jnp.asarray(table)[lax.axis_index(AXES)]
    r1 = jnp.where(diagonal, quad, r1)
    r2 = jnp.where(diagonal, corner + r2, r2)
    r1 = jnp.where(me[0] == 1, r1.T, r1)
    r2 = jnp.where(me[2] == 1, r2.T, r2)
    first = me[1] == 0
    summed = jnp.concatenate([jnp.where(first, r1, r2), jnp.where(first, r2, r1)], axis=1)
    return summed / total


def solution(mesh):
    torus = Mesh(mesh.devices.reshape(SIZES), AXES)
    mp = (ZL, X)
    placed = (P(SEQ, mp), P(None, mp), P(mp), P(SEQ), P(SEQ))

    return jax.shard_map(on_device, mesh=torus, in_specs=placed, out_specs=P(SEQ, mp), check_vma=False)
```

```python
import jax
import jax.numpy as jnp
import numpy as np
from jax import lax
from jax.experimental import pallas as pl
from jax.experimental.pallas import tpu as pltpu
from jax.sharding import Mesh
from jax.sharding import PartitionSpec as P


ZH, YW, YA, CORE, ZL, X = AXES = ("zh", "yw", "ya", "core", "zl", "x")
SIZES = (2, 2, 4, 2, 4, 4)
SEQ = (ZH, YW, YA, CORE)
CHIPS = (ZH, YW, YA)
TAU = (2, 3, 1, 0)
HALF = 128


def delivery():
    def number(seq_chip, core, mp):
        return (seq_chip * 2 + core) * 16 + mp

    edges = []
    for seq_chip in range(16):
        for h in range(2):
            for mp in range(16):
                zeta, a = divmod(seq_chip, 4)
                z, x = divmod(mp, 4)
                row = 4 * z + a
                if zeta == z:
                    col, hc = 4 * z + x, (h if a >= x else 1 - h)
                elif zeta == z ^ 1:
                    col, hc = 4 * (z ^ 1) + x, (h if z % 2 else 1 - h)
                else:
                    col, hc = 4 * TAU[z] + x, (0 if zeta == z ^ 2 else 1)
                src = number(seq_chip, h, mp)
                if row == col:
                    continue
                edges.append((src, number(row, h, col), hc, 0))
                edges.append((src, number(col, hc, row), h, 1))
    by_src, by_dst = {}, {}
    for e, (s, d, _, _) in enumerate(edges):
        by_src.setdefault(s, []).append(e)
        by_dst.setdefault(d, []).append(e)
    colour = {}
    for first in range(len(edges)):
        e = first
        while e not in colour:
            colour[e] = 0
            s = edges[e][0]
            other = [k for k in by_src[s] if k != e][0]
            colour[other] = 1
            d = edges[other][1]
            e = [k for k in by_dst[d] if k != other][0]
    pairs = ([], [])
    table = np.zeros((512, 4), np.int32)
    for e, (s, d, half, turned) in enumerate(edges):
        k = colour[e]
        pairs[k].append((s, d))
        table[d, 2 * k] = turned
        table[d, 2 * k + 1] = half
    for mp in range(16):
        for h in range(2):
            own, other = number(mp, h, mp), number(mp, 1 - h, mp)
            pairs[1].append((own, other))
            table[own] = (0, h, h, 1 - h)
    return pairs, table


def flipped(x, axis, bit=1):
    n = lax.axis_size(axis)
    return lax.ppermute(x, axis, [(i, i ^ bit) for i in range(n)])


def products(where_ref, rows, own, c1, ct, keep, send):
    x, z, core = where_ref[0], where_ref[1], where_ref[2]
    dims = (((0,), (0,)), ((), ()))
    for a in range(4):

        def put(zeta, q0, q1):
            slot = zeta * 4 + a
            keep[slot] = jnp.where(core == 0, q0, q1)
            send[slot] = jnp.where(core == 0, q1, q0)

        lhs = rows[a]
        for k, c in enumerate((own, c1, ct)):
            p = lax.dot_general(lhs, c[...], dims, preferred_element_type=jnp.float32)
            p00, p01, p10, p11 = p[:HALF, :HALF], p[:HALF, HALF:], p[HALF:, :HALF], p[HALF:, HALF:]
            if k < 2:
                same = (a >= x) if k == 0 else (lax.rem(z, 2) == 1)
                put(z if k == 0 else z ^ 1, jnp.where(same, p00, p01), jnp.where(same, p11, p10))
            else:
                put(z ^ 2, p00, p10)
                put(z ^ 3, p01, p11)


def all_products(where, rows, own, c1, ct):
    shape = jax.ShapeDtypeStruct((16, HALF, HALF), jnp.float32)
    vmem = pl.BlockSpec(memory_space=pltpu.VMEM)
    return pl.pallas_call(
        products,
        out_shape=(shape, shape),
        in_specs=[pl.BlockSpec(memory_space=pltpu.SMEM)] + [vmem] * 4,
        out_specs=(vmem, vmem),
        compiler_params=pltpu.CompilerParams(vmem_limit_bytes=16 << 20),
        cost_estimate=pl.CostEstimate(flops=2 * 1024 * 1024 * 768, bytes_accessed=5 << 20, transcendentals=0),
        name="products",
    )(where, rows, own, c1, ct)


def causal_conv(extended, weights, bias, position, doc_start, counted, length):
    taps = weights.shape[0]
    summed = jnp.zeros((length, weights.shape[1]), jnp.float32) + bias.astype(jnp.float32)
    for lag in range(taps):
        window = extended[taps - 1 - lag : taps - 1 - lag + length].astype(jnp.float32)
        usable = position - lag >= doc_start
        summed = summed + jnp.where(usable[:, None], weights[lag].astype(jnp.float32) * window, 0.0)
    return jnp.where(counted[:, None], jax.nn.silu(summed), 0.0).astype(jnp.bfloat16)


def on_device(inputs, conv_weight, conv_bias, doc_start, counts):
    pairs, table = delivery()
    length, width = inputs.shape
    taps = conv_weight.shape[0]
    core, z, x = lax.axis_index(CORE), lax.axis_index(ZL), lax.axis_index(X)
    chip = lax.axis_index(CHIPS)

    count = counts[0]
    tail = jnp.concatenate(
        [
            inputs[length - (taps - 1) :],
            jnp.full((1, width), (count // 32).astype(jnp.bfloat16)),
            jnp.full((1, width), (count % 32).astype(jnp.bfloat16)),
        ],
        axis=0,
    )
    shards = lax.axis_size(SEQ)
    prior = lax.ppermute(tail, SEQ, [(i, (i + 1) % shards) for i in range(shards)])
    count_pair = (
        count.astype(jnp.float32)
        + prior[taps - 1, 0].astype(jnp.float32) * 32.0
        + prior[taps, 0].astype(jnp.float32)
    )
    position = lax.axis_index(SEQ) * length + jnp.arange(length, dtype=jnp.int32)
    counted = jnp.arange(length, dtype=jnp.int32) < count
    extended = jnp.concatenate([prior[: taps - 1], inputs], axis=0)
    own = causal_conv(extended, conv_weight, conv_bias, position, doc_start, counted, length)

    ct = lax.ppermute(own, ZL, [(TAU[i], i) for i in range(4)])
    rows = lax.all_to_all(jnp.broadcast_to(own, (4, length, width)), X, split_axis=0, concat_axis=0, tiled=True)
    c1 = flipped(own, ZL)

    corner = lax.dot_general(
        own[:, :HALF], own[:, HALF:], (((0,), (0,)), ((), ())), preferred_element_type=jnp.float32
    )
    early = jnp.concatenate([corner, jnp.full((8, HALF), count_pair)], axis=0)
    early = early + flipped(early, YA)
    early = early + flipped(early, YA, 2)
    early = early + flipped(early, YW)
    rows, c1, ct, early = lax.optimization_barrier((rows, c1, ct, early))

    where = jnp.stack([x, z, core]).astype(jnp.int32)
    keep, send = all_products(where, rows, own, c1, ct)
    mine = keep + flipped(send, CORE)
    quad = lax.all_to_all(mine, CHIPS, split_axis=0, concat_axis=0, tiled=True)
    early = early + flipped(early, ZH)
    quad, early = lax.optimization_barrier((quad, early))
    quad = quad.sum(axis=0)
    corner, total = early[:HALF], early[HALF, 0]

    diagonal = chip == 4 * z + x
    second = lax.optimization_barrier(jnp.where(diagonal, corner, quad))
    r1 = lax.ppermute(quad, AXES, pairs[0])
    r2 = lax.ppermute(second, AXES, pairs[1])
    r1, r2 = lax.optimization_barrier((r1, r2))
    me = jnp.asarray(table)[lax.axis_index(AXES)]
    r1 = jnp.where(diagonal, quad, r1)
    r2 = jnp.where(diagonal, corner + r2, r2)
    r1 = jnp.where(me[0] == 1, r1.T, r1)
    r2 = jnp.where(me[2] == 1, r2.T, r2)
    first = me[1] == 0
    summed = jnp.concatenate([jnp.where(first, r1, r2), jnp.where(first, r2, r1)], axis=1)
    return summed / total


def solution(mesh):
    torus = Mesh(mesh.devices.reshape(SIZES), AXES)
    mp = (ZL, X)
    placed = (P(SEQ, mp), P(None, mp), P(mp), P(SEQ), P(SEQ))

    return jax.shard_map(on_device, mesh=torus, in_specs=placed, out_specs=P(SEQ, mp), check_vma=False)
```

```python
import jax
import jax.numpy as jnp
import numpy as np
from jax import lax
from jax.experimental import pallas as pl
from jax.experimental.pallas import tpu as pltpu
from jax.sharding import Mesh
from jax.sharding import PartitionSpec as P


ZH, YW, YA, CORE, ZL, X = AXES = ("zh", "yw", "ya", "core", "zl", "x")
SIZES = (2, 2, 4, 2, 4, 4)
SEQ = (ZH, YW, YA, CORE)
CHIPS = (ZH, YW, YA)
TAU = (2, 3, 1, 0)
HALF = 128
EXTRA = 8


def delivery():
    def number(seq_chip, core, mp):
        return (seq_chip * 2 + core) * 16 + mp

    edges = []
    for seq_chip in range(16):
        for h in range(2):
            for mp in range(16):
                zeta, a = divmod(seq_chip, 4)
                z, x = divmod(mp, 4)
                row = 4 * z + a
                if zeta == z:
                    col, hc = 4 * z + x, (h if a >= x else 1 - h)
                elif zeta == z ^ 1:
                    col, hc = 4 * (z ^ 1) + x, (h if z % 2 else 1 - h)
                else:
                    col, hc = 4 * TAU[z] + x, (0 if zeta == z ^ 2 else 1)
                src = number(seq_chip, h, mp)
                if row == col:
                    continue
                edges.append((src, number(row, h, col), hc, 0))
                edges.append((src, number(col, hc, row), h, 1))
    by_src, by_dst = {}, {}
    for e, (s, d, _, _) in enumerate(edges):
        by_src.setdefault(s, []).append(e)
        by_dst.setdefault(d, []).append(e)
    colour = {}
    for first in range(len(edges)):
        e = first
        while e not in colour:
            colour[e] = 0
            s = edges[e][0]
            other = [k for k in by_src[s] if k != e][0]
            colour[other] = 1
            d = edges[other][1]
            e = [k for k in by_dst[d] if k != other][0]
    pairs = ([], [])
    table = np.zeros((512, 4), np.int32)
    for e, (s, d, half, turned) in enumerate(edges):
        k = colour[e]
        pairs[k].append((s, d))
        table[d, 2 * k] = turned
        if k == 0:
            table[d, 1] = half
    for mp in range(16):
        for h in range(2):
            own, other = number(mp, h, mp), number(mp, 1 - h, mp)
            pairs[1].append((own, other))
            table[own] = (0, h, 0, 1)
    return pairs, table


def flipped(x, axis, bit=1):
    n = lax.axis_size(axis)
    return lax.ppermute(x, axis, [(i, i ^ bit) for i in range(n)])


def products(where_ref, rows, own, c1, ct, keep, send):
    x, z, core, count = where_ref[0], where_ref[1], where_ref[2], where_ref[3]
    dims = (((0,), (0,)), ((), ()))
    r = lax.broadcasted_iota(jnp.int32, (HALF, HALF), 0)
    c = lax.broadcasted_iota(jnp.int32, (HALF, HALF), 1)
    extra_row = lax.broadcasted_iota(jnp.int32, (EXTRA, HALF), 0)
    counted = jnp.where(extra_row == 1, count.astype(jnp.float32), 0.0)
    for a in range(4):

        def put(zeta, q0, q1):
            slot = zeta * 4 + a
            keep[slot, :HALF] = jnp.where(core == 0, q0, q1)
            send[slot, :HALF] = jnp.where(core == 0, q1, q0)
            keep[slot, HALF:] = counted
            send[slot, HALF:] = counted

        lhs = rows[a]
        for k, block in enumerate((own, c1, ct)):
            p = lax.dot_general(lhs, block[...], dims, preferred_element_type=jnp.float32)
            p00, p01, p10, p11 = p[:HALF, :HALF], p[:HALF, HALF:], p[HALF:, :HALF], p[HALF:, HALF:]
            if k == 0:
                reach = jnp.where(a > x, HALF, jnp.where(a == x, 0, -HALF))
                same = r - c <= reach
                put(z, jnp.where(same, p00, p01), jnp.where(same, p11, p10))
                middle = jnp.sum(jnp.where((r == c) & (a == x), p01, 0.0), axis=0, keepdims=True)
                middle = jnp.where(extra_row == 0, middle, counted)
                keep[z * 4 + a, HALF:] = middle
                send[z * 4 + a, HALF:] = middle
            elif k == 1:
                same = lax.rem(z, 2) == 1
                put(z ^ 1, jnp.where(same, p00, p01), jnp.where(same, p11, p10))
            else:
                put(z ^ 2, p00, p10)
                put(z ^ 3, p01, p11)


def all_products(where, rows, own, c1, ct):
    shape = jax.ShapeDtypeStruct((16, HALF + EXTRA, HALF), jnp.float32)
    vmem = pl.BlockSpec(memory_space=pltpu.VMEM)
    return pl.pallas_call(
        products,
        out_shape=(shape, shape),
        in_specs=[pl.BlockSpec(memory_space=pltpu.SMEM)] + [vmem] * 4,
        out_specs=(vmem, vmem),
        compiler_params=pltpu.CompilerParams(vmem_limit_bytes=16 << 20),
        cost_estimate=pl.CostEstimate(flops=2 * 1024 * 1024 * 768, bytes_accessed=5 << 20, transcendentals=0),
        name="products",
    )(where, rows, own, c1, ct)


def assemble(how, quad, extra, r1, r2, out):
    turn1, half1, turn2, diagonal = how[0] == 1, how[1], how[2] == 1, how[3] == 1
    r = lax.broadcasted_iota(jnp.int32, (HALF, HALF), 0)
    c = lax.broadcasted_iota(jnp.int32, (HALF, HALF), 1)
    m, got1, got2 = quad[...], r1[...], r2[...]
    turned2 = got2.T
    own = jnp.where(r <= c, m, m.T)
    cross = jnp.where(r > c, m, jnp.where(r == c, extra[0:1], turned2))
    q1 = jnp.where(diagonal, own, jnp.where(turn1, got1.T, got1))
    q2 = jnp.where(diagonal, cross, jnp.where(turn2, turned2, got2))
    total = extra[1:2]
    out[:, :HALF] = jnp.where(half1 == 0, q1, q2) / total
    out[:, HALF:] = jnp.where(half1 == 0, q2, q1) / total


def assembled(how, quad, extra, r1, r2):
    vmem = pl.BlockSpec(memory_space=pltpu.VMEM)
    return pl.pallas_call(
        assemble,
        out_shape=jax.ShapeDtypeStruct((HALF, 2 * HALF), jnp.float32),
        in_specs=[pl.BlockSpec(memory_space=pltpu.SMEM)] + [vmem] * 4,
        out_specs=vmem,
        compiler_params=pltpu.CompilerParams(vmem_limit_bytes=4 << 20),
        cost_estimate=pl.CostEstimate(flops=1 << 20, bytes_accessed=1 << 19, transcendentals=0),
        name="assemble",
    )(how, quad, extra, r1, r2)


def causal_conv(extended, weights, bias, position, doc_start, counted, length):
    taps = weights.shape[0]
    summed = jnp.zeros((length, weights.shape[1]), jnp.float32) + bias.astype(jnp.float32)
    for lag in range(taps):
        window = extended[taps - 1 - lag : taps - 1 - lag + length].astype(jnp.float32)
        usable = position - lag >= doc_start
        summed = summed + jnp.where(usable[:, None], weights[lag].astype(jnp.float32) * window, 0.0)
    return jnp.where(counted[:, None], jax.nn.silu(summed), 0.0).astype(jnp.bfloat16)


def on_device(inputs, conv_weight, conv_bias, doc_start, counts):
    pairs, table = delivery()
    length, width = inputs.shape
    taps = conv_weight.shape[0]
    core, z, x = lax.axis_index(CORE), lax.axis_index(ZL), lax.axis_index(X)
    count = counts[0]

    shards = lax.axis_size(SEQ)
    prior = lax.ppermute(inputs[length - (taps - 1) :], SEQ, [(i, (i + 1) % shards) for i in range(shards)])
    position = lax.axis_index(SEQ) * length + jnp.arange(length, dtype=jnp.int32)
    counted = jnp.arange(length, dtype=jnp.int32) < count
    extended = jnp.concatenate([prior, inputs], axis=0)
    own = causal_conv(extended, conv_weight, conv_bias, position, doc_start, counted, length)

    ct = lax.ppermute(own, ZL, [(TAU[i], i) for i in range(4)])
    rows = lax.all_to_all(jnp.broadcast_to(own, (4, length, width)), X, split_axis=0, concat_axis=0, tiled=True)
    c1 = flipped(own, ZL)

    where = jnp.stack([x, z, core, count]).astype(jnp.int32)
    keep, send = all_products(where, rows, own, c1, ct)
    mine = keep + flipped(send, CORE)
    summed = lax.all_to_all(mine, CHIPS, split_axis=0, concat_axis=0, tiled=True).sum(axis=0)
    quad, extra = summed[:HALF], summed[HALF:]

    r1 = lax.ppermute(quad, AXES, pairs[0])
    r2 = lax.ppermute(quad, AXES, pairs[1])
    how = lax.dynamic_index_in_dim(jnp.asarray(table), lax.axis_index(AXES), keepdims=False)
    return assembled(how, quad, extra, r1, r2)


def solution(mesh):
    torus = Mesh(mesh.devices.reshape(SIZES), AXES)
    mp = (ZL, X)
    placed = (P(SEQ, mp), P(None, mp), P(mp), P(SEQ), P(SEQ))

    return jax.shard_map(on_device, mesh=torus, in_specs=placed, out_specs=P(SEQ, mp), check_vma=False)
```

```python
import jax
import jax.numpy as jnp
import numpy as np
from jax import lax
from jax.experimental import pallas as pl
from jax.experimental.pallas import tpu as pltpu
from jax.sharding import Mesh
from jax.sharding import PartitionSpec as P


ZH, YW, YA, CORE, ZL, X = AXES = ("zh", "yw", "ya", "core", "zl", "x")
SIZES = (2, 2, 4, 2, 4, 4)
SEQ = (ZH, YW, YA, CORE)
CHIPS = (ZH, YW, YA)
TAU = (2, 3, 1, 0)
HALF = 128
EXTRA = 8


def delivery():
    def number(seq_chip, core, mp):
        return (seq_chip * 2 + core) * 16 + mp

    edges = []
    for seq_chip in range(16):
        for h in range(2):
            for mp in range(16):
                zeta, a = divmod(seq_chip, 4)
                z, x = divmod(mp, 4)
                row = 4 * z + a
                if zeta == z:
                    col, hc = 4 * z + x, (h if a >= x else 1 - h)
                elif zeta == z ^ 1:
                    col, hc = 4 * (z ^ 1) + x, (h if z % 2 else 1 - h)
                else:
                    col, hc = 4 * TAU[z] + x, (0 if zeta == z ^ 2 else 1)
                src = number(seq_chip, h, mp)
                if row == col:
                    continue
                edges.append((src, number(row, h, col), hc, 0))
                edges.append((src, number(col, hc, row), h, 1))
    by_src, by_dst = {}, {}
    for e, (s, d, _, _) in enumerate(edges):
        by_src.setdefault(s, []).append(e)
        by_dst.setdefault(d, []).append(e)
    colour = {}
    for first in range(len(edges)):
        e = first
        while e not in colour:
            colour[e] = 0
            s = edges[e][0]
            other = [k for k in by_src[s] if k != e][0]
            colour[other] = 1
            d = edges[other][1]
            e = [k for k in by_dst[d] if k != other][0]
    pairs = ([], [])
    table = np.zeros((512, 4), np.int32)
    for e, (s, d, half, turned) in enumerate(edges):
        k = colour[e]
        pairs[k].append((s, d))
        table[d, 2 * k] = turned
        if k == 0:
            table[d, 1] = half
    for mp in range(16):
        for h in range(2):
            own, other = number(mp, h, mp), number(mp, 1 - h, mp)
            pairs[1].append((own, other))
            table[own] = (0, h, 0, 1)
    return pairs, table


def flipped(x, axis, bit=1):
    n = lax.axis_size(axis)
    return lax.ppermute(x, axis, [(i, i ^ bit) for i in range(n)])


def products(where_ref, rows, own, c1, ct, keep, send):
    x, z, core, count = where_ref[0], where_ref[1], where_ref[2], where_ref[3]
    dims = (((0,), (0,)), ((), ()))
    r = lax.broadcasted_iota(jnp.int32, (HALF, HALF), 0)
    c = lax.broadcasted_iota(jnp.int32, (HALF, HALF), 1)
    extra_row = lax.broadcasted_iota(jnp.int32, (EXTRA, HALF), 0)
    counted = jnp.where(extra_row == 1, count.astype(jnp.float32), 0.0)
    for a in range(4):

        def put(zeta, q0, q1):
            slot = zeta * 4 + a
            keep[slot, :HALF] = jnp.where(core == 0, q0, q1)
            send[slot, :HALF] = jnp.where(core == 0, q1, q0)
            keep[slot, HALF:] = counted
            send[slot, HALF:] = counted

        lhs = rows[a]
        for k, block in enumerate((own, c1, ct)):
            p = lax.dot_general(lhs, block[...], dims, preferred_element_type=jnp.float32)
            p00, p01, p10, p11 = p[:HALF, :HALF], p[:HALF, HALF:], p[HALF:, :HALF], p[HALF:, HALF:]
            if k == 0:
                reach = jnp.where(a > x, HALF, jnp.where(a == x, 0, -HALF))
                same = r - c <= reach
                put(z, jnp.where(same, p00, p01), jnp.where(same, p11, p10))
                middle = jnp.sum(jnp.where((r == c) & (a == x), p01, 0.0), axis=0, keepdims=True)
                middle = jnp.where(extra_row == 0, middle, counted)
                keep[z * 4 + a, HALF:] = middle
                send[z * 4 + a, HALF:] = middle
            elif k == 1:
                same = lax.rem(z, 2) == 1
                put(z ^ 1, jnp.where(same, p00, p01), jnp.where(same, p11, p10))
            else:
                put(z ^ 2, p00, p10)
                put(z ^ 3, p01, p11)


def all_products(where, rows, own, c1, ct):
    shape = jax.ShapeDtypeStruct((16, HALF + EXTRA, HALF), jnp.float32)
    vmem = pl.BlockSpec(memory_space=pltpu.VMEM)
    return pl.pallas_call(
        products,
        out_shape=(shape, shape),
        in_specs=[pl.BlockSpec(memory_space=pltpu.SMEM)] + [vmem] * 4,
        out_specs=(vmem, vmem),
        compiler_params=pltpu.CompilerParams(vmem_limit_bytes=16 << 20),
        cost_estimate=pl.CostEstimate(flops=2 * 1024 * 1024 * 768, bytes_accessed=5 << 20, transcendentals=0),
        name="products",
    )(where, rows, own, c1, ct)


def assemble(how, quad, extra, r1, r2, out):
    turn1, half1, turn2, diagonal = how[0] == 1, how[1], how[2] == 1, how[3] == 1
    r = lax.broadcasted_iota(jnp.int32, (HALF, HALF), 0)
    c = lax.broadcasted_iota(jnp.int32, (HALF, HALF), 1)
    m, got1, got2 = quad[...], r1[...], r2[...]
    turned2 = got2.T
    own = jnp.where(r <= c, m, m.T)
    cross = jnp.where(r > c, m, jnp.where(r == c, extra[0:1], turned2))
    q1 = jnp.where(diagonal, own, jnp.where(turn1, got1.T, got1))
    q2 = jnp.where(diagonal, cross, jnp.where(turn2, turned2, got2))
    total = extra[1:2]
    out[:, :HALF] = jnp.where(half1 == 0, q1, q2) / total
    out[:, HALF:] = jnp.where(half1 == 0, q2, q1) / total


def assembled(how, quad, extra, r1, r2):
    vmem = pl.BlockSpec(memory_space=pltpu.VMEM)
    return pl.pallas_call(
        assemble,
        out_shape=jax.ShapeDtypeStruct((HALF, 2 * HALF), jnp.float32),
        in_specs=[pl.BlockSpec(memory_space=pltpu.SMEM)] + [vmem] * 4,
        out_specs=vmem,
        compiler_params=pltpu.CompilerParams(vmem_limit_bytes=4 << 20),
        cost_estimate=pl.CostEstimate(flops=1 << 20, bytes_accessed=1 << 19, transcendentals=0),
        name="assemble",
    )(how, quad, extra, r1, r2)


def activated(window_of, code, weights, bias):
    v = bias[...].astype(jnp.float32)
    for lag in range(weights.shape[0]):
        term = weights[lag : lag + 1, :].astype(jnp.float32) * window_of(lag)
        v = v + jnp.where(code >= lag, term, 0.0)
    return jnp.where(code >= 0, v * (1.0 / (1.0 + jnp.exp(-v))), 0.0)


def codes(group, doc_start, counts):
    token = group * HALF + lax.broadcasted_iota(jnp.int32, (1, HALF), 1)
    place = lax.axis_index(SEQ) * (8 * HALF) + token
    age = jnp.minimum(place - doc_start[group : group + 1, :], 3)
    code = jnp.where(token < counts[0], age, -1).astype(jnp.float32)
    column = jnp.broadcast_to(code, (HALF, HALF)).T
    return jnp.concatenate([column, column], axis=1)


def conv_body(counts, inputs, weights, bias, doc_start, out, lead):
    lead[...] = inputs[:16, :]
    for group in range(8):
        base = group * HALF
        code = codes(group, doc_start, counts)
        if group:
            wide = inputs[base - 16 : base + HALF, :].astype(jnp.float32)
        else:
            wide = jnp.concatenate([jnp.zeros((16, 2 * HALF), jnp.float32), inputs[:HALF, :].astype(jnp.float32)], axis=0)
        value = activated(lambda lag: wide[16 - lag : 16 - lag + HALF], code, weights, bias)
        out[base : base + HALF, :] = value.astype(jnp.bfloat16)


def head_body(counts, main, lead, prior, weights, bias, doc_start, own, copies):
    code = codes(0, doc_start, counts)[:16]
    wide = jnp.concatenate([prior[...].astype(jnp.float32), lead[...].astype(jnp.float32)], axis=0)
    value = activated(lambda lag: wide[8 - lag : 24 - lag], code, weights, bias)
    head = value.astype(jnp.bfloat16)
    rest = main[16:, :]
    own[:16, :] = head
    own[16:, :] = rest
    for k in range(4):
        copies[k, :16, :] = head
        copies[k, 16:, :] = rest


VMEM = pl.BlockSpec(memory_space=pltpu.VMEM)
SMEM = pl.BlockSpec(memory_space=pltpu.SMEM)


def conv_main(counts, inputs, weights, bias, doc_start):
    return pl.pallas_call(
        conv_body,
        out_shape=(
            jax.ShapeDtypeStruct(inputs.shape, jnp.bfloat16),
            jax.ShapeDtypeStruct((16, inputs.shape[1]), jnp.bfloat16),
        ),
        in_specs=[SMEM] + [VMEM] * 4,
        out_specs=(VMEM, VMEM),
        compiler_params=pltpu.CompilerParams(vmem_limit_bytes=8 << 20),
        cost_estimate=pl.CostEstimate(flops=8 << 20, bytes_accessed=1 << 20, transcendentals=1 << 19),
        name="conv_main",
    )(counts, inputs, weights, bias, doc_start)


def conv_head(counts, main, lead, prior, weights, bias, doc_start):
    shape = jax.ShapeDtypeStruct(main.shape, jnp.bfloat16)
    return pl.pallas_call(
        head_body,
        out_shape=(shape, jax.ShapeDtypeStruct((4, *main.shape), jnp.bfloat16)),
        in_specs=[SMEM] + [VMEM] * 6,
        out_specs=(VMEM, VMEM),
        compiler_params=pltpu.CompilerParams(vmem_limit_bytes=8 << 20),
        cost_estimate=pl.CostEstimate(flops=1 << 20, bytes_accessed=1 << 20, transcendentals=0),
        name="conv_head",
    )(counts, main, lead, prior, weights, bias, doc_start)


def on_device(inputs, conv_weight, conv_bias, doc_start, counts):
    pairs, table = delivery()
    length, width = inputs.shape
    core, z, x = lax.axis_index(CORE), lax.axis_index(ZL), lax.axis_index(X)
    count = counts[0]

    shards = lax.axis_size(SEQ)
    prior = lax.ppermute(inputs[length - 8 :], SEQ, [(i, i + 1) for i in range(shards - 1)])
    bias, starts = conv_bias.reshape(1, width), doc_start.reshape(8, HALF)
    main, lead = conv_main(counts, inputs, conv_weight, bias, starts)
    own, copies = conv_head(counts, main, lead, prior, conv_weight, bias, starts)

    ct = lax.ppermute(own, ZL, [(TAU[i], i) for i in range(4)])
    rows = lax.all_to_all(copies, X, split_axis=0, concat_axis=0, tiled=True)
    c1 = flipped(own, ZL)

    where = jnp.stack([x, z, core, count]).astype(jnp.int32)
    keep, send = all_products(where, rows, own, c1, ct)
    mine = keep + flipped(send, CORE)
    summed = lax.all_to_all(mine, CHIPS, split_axis=0, concat_axis=0, tiled=True).sum(axis=0)
    quad, extra = summed[:HALF], summed[HALF:]

    r1 = lax.ppermute(quad, AXES, pairs[0])
    r2 = lax.ppermute(quad, AXES, pairs[1])
    how = lax.dynamic_index_in_dim(jnp.asarray(table), lax.axis_index(AXES), keepdims=False)
    return assembled(how, quad, extra, r1, r2)


def solution(mesh):
    torus = Mesh(mesh.devices.reshape(SIZES), AXES)
    mp = (ZL, X)
    placed = (P(SEQ, mp), P(None, mp), P(mp), P(SEQ), P(SEQ))

    return jax.shard_map(on_device, mesh=torus, in_specs=placed, out_specs=P(SEQ, mp), check_vma=False)
```

```python
import jax
import jax.numpy as jnp
import numpy as np
from jax import lax
from jax.experimental import pallas as pl
from jax.experimental.pallas import tpu as pltpu
from jax.sharding import Mesh
from jax.sharding import PartitionSpec as P


ZH, YW, YA, CORE, ZL, X = AXES = ("zh", "yw", "ya", "core", "zl", "x")
SIZES = (2, 2, 4, 2, 4, 4)
SEQ = (ZH, YW, YA, CORE)
CHIPS = (ZH, YW, YA)
TAU = (2, 3, 1, 0)
HALF = 128
EXTRA = 8
PACK = 16
LEVELS = 32767.0
VMEM = pl.BlockSpec(memory_space=pltpu.VMEM)
SMEM = pl.BlockSpec(memory_space=pltpu.SMEM)


def delivery():
    def number(seq_chip, core, mp):
        return (seq_chip * 2 + core) * 16 + mp

    edges = []
    for seq_chip in range(16):
        for h in range(2):
            for mp in range(16):
                zeta, a = divmod(seq_chip, 4)
                z, x = divmod(mp, 4)
                row = 4 * z + a
                if zeta == z:
                    col, hc = 4 * z + x, (h if a >= x else 1 - h)
                elif zeta == z ^ 1:
                    col, hc = 4 * (z ^ 1) + x, (h if z % 2 else 1 - h)
                else:
                    col, hc = 4 * TAU[z] + x, (0 if zeta == z ^ 2 else 1)
                src = number(seq_chip, h, mp)
                if row == col:
                    continue
                edges.append((src, number(row, h, col), hc, 0))
                edges.append((src, number(col, hc, row), h, 1))
    by_src, by_dst = {}, {}
    for e, (s, d, _, _) in enumerate(edges):
        by_src.setdefault(s, []).append(e)
        by_dst.setdefault(d, []).append(e)
    colour = {}
    for first in range(len(edges)):
        e = first
        while e not in colour:
            colour[e] = 0
            s = edges[e][0]
            other = [k for k in by_src[s] if k != e][0]
            colour[other] = 1
            d = edges[other][1]
            e = [k for k in by_dst[d] if k != other][0]
    pairs = ([], [])
    table = np.zeros((512, 4), np.int32)
    for e, (s, d, half, turned) in enumerate(edges):
        k = colour[e]
        pairs[k].append((s, d))
        table[d, 2 * k] = turned
        if k == 0:
            table[d, 1] = half
    for mp in range(16):
        for h in range(2):
            own, other = number(mp, h, mp), number(mp, 1 - h, mp)
            pairs[1].append((own, other))
            table[own] = (0, h, 0, 1)
    return pairs, table


def flipped(x, axis, bit=1):
    n = lax.axis_size(axis)
    return lax.ppermute(x, axis, [(i, i ^ bit) for i in range(n)])


def products(where_ref, rows, own, c1, ct, keep, send):
    x, z, core, count = where_ref[0], where_ref[1], where_ref[2], where_ref[3]
    dims = (((0,), (0,)), ((), ()))
    r = lax.broadcasted_iota(jnp.int32, (HALF, HALF), 0)
    c = lax.broadcasted_iota(jnp.int32, (HALF, HALF), 1)
    extra_row = lax.broadcasted_iota(jnp.int32, (EXTRA, HALF), 0)
    counted = jnp.where(extra_row == 1, count.astype(jnp.float32), 0.0)
    for a in range(4):

        def put(zeta, q0, q1):
            slot = zeta * 4 + a
            keep[slot, :HALF] = jnp.where(core == 0, q0, q1)
            send[slot, :HALF] = jnp.where(core == 0, q1, q0)
            keep[slot, HALF:] = counted
            send[slot, HALF:] = counted

        lhs = rows[a]
        for k, block in enumerate((own, c1, ct)):
            p = lax.dot_general(lhs, block[...], dims, preferred_element_type=jnp.float32)
            p00, p01, p10, p11 = p[:HALF, :HALF], p[:HALF, HALF:], p[HALF:, :HALF], p[HALF:, HALF:]
            if k == 0:
                reach = jnp.where(a > x, HALF, jnp.where(a == x, 0, -HALF))
                same = r - c <= reach
                put(z, jnp.where(same, p00, p01), jnp.where(same, p11, p10))
                middle = jnp.sum(jnp.where((r == c) & (a == x), p01, 0.0), axis=0, keepdims=True)
                middle = jnp.where(extra_row == 0, middle, counted)
                keep[z * 4 + a, HALF:] = middle
                send[z * 4 + a, HALF:] = middle
            elif k == 1:
                same = lax.rem(z, 2) == 1
                put(z ^ 1, jnp.where(same, p00, p01), jnp.where(same, p11, p10))
            else:
                put(z ^ 2, p00, p10)
                put(z ^ 3, p01, p11)


def all_products(where, rows, own, c1, ct):
    shape = jax.ShapeDtypeStruct((16, HALF + EXTRA, HALF), jnp.float32)
    vmem = pl.BlockSpec(memory_space=pltpu.VMEM)
    return pl.pallas_call(
        products,
        out_shape=(shape, shape),
        in_specs=[pl.BlockSpec(memory_space=pltpu.SMEM)] + [vmem] * 4,
        out_specs=(vmem, vmem),
        compiler_params=pltpu.CompilerParams(vmem_limit_bytes=16 << 20),
        cost_estimate=pl.CostEstimate(flops=2 * 1024 * 1024 * 768, bytes_accessed=5 << 20, transcendentals=0),
        name="products",
    )(where, rows, own, c1, ct)


def scale_of(code):
    return jnp.exp2(code * (1.0 / 256.0))


def encode(keep, got, out):
    row = lax.broadcasted_iota(jnp.int32, (PACK, HALF), 0)

    def one(slot, carry):
        v = keep[slot, :HALF] + got[slot, :HALF]
        extra = keep[slot, HALF:] + got[slot, HALF:]
        middle, count = extra[0:1], extra[1:2]
        most = jnp.maximum(jnp.max(jnp.abs(v), axis=0, keepdims=True), jnp.abs(middle))
        code = jnp.ceil(jnp.log2(jnp.maximum(most, 1e-37)) * 256.0)
        rate = LEVELS / scale_of(code)
        tail = jnp.where(row == 0, middle * rate, jnp.where(row == 1, code, jnp.where(row == 2, count, 0.0)))
        out[slot, :HALF] = whole(v * rate)
        out[slot, HALF:] = whole(tail)
        return carry

    lax.fori_loop(0, 16, one, 0)


def whole(v):
    return jnp.clip(jnp.round(v), -LEVELS, LEVELS).astype(jnp.int32).astype(jnp.int16)


def decode(coded, quad, extra):
    row = lax.broadcasted_iota(jnp.int32, (EXTRA, HALF), 0)

    def one(slot, carry):
        total, rest = carry
        tail = coded[slot, HALF:].astype(jnp.int32).astype(jnp.float32)
        scale = scale_of(tail[1:2]) * (1.0 / LEVELS)
        total = total + coded[slot, :HALF].astype(jnp.int32).astype(jnp.float32) * scale
        rest = rest + jnp.where(row == 0, tail[0:1] * scale, jnp.where(row == 1, tail[2:3], 0.0))
        return total, rest

    start = jnp.zeros((HALF, HALF), jnp.float32), jnp.zeros((EXTRA, HALF), jnp.float32)
    quad[...], extra[...] = lax.fori_loop(0, 16, one, start)


def encoded(keep, got):
    return pl.pallas_call(
        encode,
        out_shape=jax.ShapeDtypeStruct((16, HALF + PACK, HALF), jnp.int16),
        in_specs=[VMEM] * 2,
        out_specs=VMEM,
        compiler_params=pltpu.CompilerParams(vmem_limit_bytes=8 << 20),
        cost_estimate=pl.CostEstimate(flops=2 << 20, bytes_accessed=3 << 20, transcendentals=0),
        name="encode",
    )(keep, got)


def decoded(coded):
    return pl.pallas_call(
        decode,
        out_shape=(
            jax.ShapeDtypeStruct((HALF, HALF), jnp.float32),
            jax.ShapeDtypeStruct((EXTRA, HALF), jnp.float32),
        ),
        in_specs=[VMEM],
        out_specs=(VMEM, VMEM),
        compiler_params=pltpu.CompilerParams(vmem_limit_bytes=8 << 20),
        cost_estimate=pl.CostEstimate(flops=2 << 20, bytes_accessed=1 << 20, transcendentals=0),
        name="decode",
    )(coded)


def assemble(how, quad, extra, r1, r2, out):
    turn1, half1, turn2, diagonal = how[0] == 1, how[1], how[2] == 1, how[3] == 1
    r = lax.broadcasted_iota(jnp.int32, (HALF, HALF), 0)
    c = lax.broadcasted_iota(jnp.int32, (HALF, HALF), 1)
    m, got1, got2 = quad[...], r1[...], r2[...]
    turned2 = got2.T
    own = jnp.where(r <= c, m, m.T)
    cross = jnp.where(r > c, m, jnp.where(r == c, extra[0:1], turned2))
    q1 = jnp.where(diagonal, own, jnp.where(turn1, got1.T, got1))
    q2 = jnp.where(diagonal, cross, jnp.where(turn2, turned2, got2))
    total = extra[1:2]
    out[:, :HALF] = jnp.where(half1 == 0, q1, q2) / total
    out[:, HALF:] = jnp.where(half1 == 0, q2, q1) / total


def assembled(how, quad, extra, r1, r2):
    vmem = pl.BlockSpec(memory_space=pltpu.VMEM)
    return pl.pallas_call(
        assemble,
        out_shape=jax.ShapeDtypeStruct((HALF, 2 * HALF), jnp.float32),
        in_specs=[pl.BlockSpec(memory_space=pltpu.SMEM)] + [vmem] * 4,
        out_specs=vmem,
        compiler_params=pltpu.CompilerParams(vmem_limit_bytes=4 << 20),
        cost_estimate=pl.CostEstimate(flops=1 << 20, bytes_accessed=1 << 19, transcendentals=0),
        name="assemble",
    )(how, quad, extra, r1, r2)


def activated(window_of, code, weights, bias):
    v = bias[...].astype(jnp.float32)
    for lag in range(weights.shape[0]):
        term = weights[lag : lag + 1, :].astype(jnp.float32) * window_of(lag)
        v = v + jnp.where(code >= lag, term, 0.0)
    return jnp.where(code >= 0, v * (1.0 / (1.0 + jnp.exp(-v))), 0.0)


def codes(group, doc_start, counts):
    token = group * HALF + lax.broadcasted_iota(jnp.int32, (1, HALF), 1)
    place = lax.axis_index(SEQ) * (8 * HALF) + token
    age = jnp.minimum(place - doc_start[group : group + 1, :], 3)
    code = jnp.where(token < counts[0], age, -1).astype(jnp.float32)
    column = jnp.broadcast_to(code, (HALF, HALF)).T
    return jnp.concatenate([column, column], axis=1)


def conv_body(counts, inputs, weights, bias, doc_start, out, lead):
    lead[...] = inputs[:16, :]
    for group in range(8):
        base = group * HALF
        code = codes(group, doc_start, counts)
        if group:
            wide = inputs[base - 16 : base + HALF, :].astype(jnp.float32)
        else:
            wide = jnp.concatenate([jnp.zeros((16, 2 * HALF), jnp.float32), inputs[:HALF, :].astype(jnp.float32)], axis=0)
        value = activated(lambda lag: wide[16 - lag : 16 - lag + HALF], code, weights, bias)
        out[base : base + HALF, :] = value.astype(jnp.bfloat16)


def head_body(counts, main, lead, prior, weights, bias, doc_start, own, copies):
    code = codes(0, doc_start, counts)[:16]
    wide = jnp.concatenate([prior[...].astype(jnp.float32), lead[...].astype(jnp.float32)], axis=0)
    value = activated(lambda lag: wide[8 - lag : 24 - lag], code, weights, bias)
    head = value.astype(jnp.bfloat16)
    rest = main[16:, :]
    own[:16, :] = head
    own[16:, :] = rest
    for k in range(4):
        copies[k, :16, :] = head
        copies[k, 16:, :] = rest


def conv_main(counts, inputs, weights, bias, doc_start):
    return pl.pallas_call(
        conv_body,
        out_shape=(
            jax.ShapeDtypeStruct(inputs.shape, jnp.bfloat16),
            jax.ShapeDtypeStruct((16, inputs.shape[1]), jnp.bfloat16),
        ),
        in_specs=[SMEM] + [VMEM] * 4,
        out_specs=(VMEM, VMEM),
        compiler_params=pltpu.CompilerParams(vmem_limit_bytes=8 << 20),
        cost_estimate=pl.CostEstimate(flops=8 << 20, bytes_accessed=1 << 20, transcendentals=1 << 19),
        name="conv_main",
    )(counts, inputs, weights, bias, doc_start)


def conv_head(counts, main, lead, prior, weights, bias, doc_start):
    shape = jax.ShapeDtypeStruct(main.shape, jnp.bfloat16)
    return pl.pallas_call(
        head_body,
        out_shape=(shape, jax.ShapeDtypeStruct((4, *main.shape), jnp.bfloat16)),
        in_specs=[SMEM] + [VMEM] * 6,
        out_specs=(VMEM, VMEM),
        compiler_params=pltpu.CompilerParams(vmem_limit_bytes=8 << 20),
        cost_estimate=pl.CostEstimate(flops=1 << 20, bytes_accessed=1 << 20, transcendentals=0),
        name="conv_head",
    )(counts, main, lead, prior, weights, bias, doc_start)


def on_device(inputs, conv_weight, conv_bias, doc_start, counts):
    pairs, table = delivery()
    length, width = inputs.shape
    core, z, x = lax.axis_index(CORE), lax.axis_index(ZL), lax.axis_index(X)
    count = counts[0]

    shards = lax.axis_size(SEQ)
    prior = lax.ppermute(inputs[length - 8 :], SEQ, [(i, i + 1) for i in range(shards - 1)])
    bias, starts = conv_bias.reshape(1, width), doc_start.reshape(8, HALF)
    main, lead = conv_main(counts, inputs, conv_weight, bias, starts)
    own, copies = conv_head(counts, main, lead, prior, conv_weight, bias, starts)

    ct = lax.ppermute(own, ZL, [(TAU[i], i) for i in range(4)])
    rows = lax.all_to_all(copies, X, split_axis=0, concat_axis=0, tiled=True)
    c1 = flipped(own, ZL)

    where = jnp.stack([x, z, core, count]).astype(jnp.int32)
    keep, send = all_products(where, rows, own, c1, ct)
    coded = encoded(keep, flipped(send, CORE))
    quad, extra = decoded(lax.all_to_all(coded, CHIPS, split_axis=0, concat_axis=0, tiled=True))

    r1 = lax.ppermute(quad, AXES, pairs[0])
    r2 = lax.ppermute(quad, AXES, pairs[1])
    how = lax.dynamic_index_in_dim(jnp.asarray(table), lax.axis_index(AXES), keepdims=False)
    return assembled(how, quad, extra, r1, r2)


def solution(mesh):
    torus = Mesh(mesh.devices.reshape(SIZES), AXES)
    mp = (ZL, X)
    placed = (P(SEQ, mp), P(None, mp), P(mp), P(SEQ), P(SEQ))

    return jax.shard_map(on_device, mesh=torus, in_specs=placed, out_specs=P(SEQ, mp), check_vma=False)
```

```python
import jax
import jax.numpy as jnp
import numpy as np
from jax import lax
from jax.experimental import pallas as pl
from jax.experimental.pallas import tpu as pltpu
from jax.sharding import Mesh
from jax.sharding import PartitionSpec as P


ZH, YW, YA, CORE, ZL, X = AXES = ("zh", "yw", "ya", "core", "zl", "x")
SIZES = (2, 2, 4, 2, 4, 4)
SEQ = (ZH, YW, YA, CORE)
CHIPS = (ZH, YW, YA)
TAU = (2, 3, 1, 0)
HALF = 128
EXTRA = 8
PACK = 16
LEVELS = 32767.0
VMEM = pl.BlockSpec(memory_space=pltpu.VMEM)
SMEM = pl.BlockSpec(memory_space=pltpu.SMEM)


def delivery():
    def number(seq_chip, core, mp):
        return (seq_chip * 2 + core) * 16 + mp

    edges = []
    for seq_chip in range(16):
        for h in range(2):
            for mp in range(16):
                zeta, a = divmod(seq_chip, 4)
                z, x = divmod(mp, 4)
                row = 4 * z + a
                if zeta == z:
                    col, hc = 4 * z + x, (h if a >= x else 1 - h)
                elif zeta == z ^ 1:
                    col, hc = 4 * (z ^ 1) + x, (h if z % 2 else 1 - h)
                else:
                    col, hc = 4 * TAU[z] + x, (0 if zeta == z ^ 2 else 1)
                src = number(seq_chip, h, mp)
                if row == col:
                    continue
                edges.append((src, number(row, h, col), hc, 0))
                edges.append((src, number(col, hc, row), h, 1))
    by_src, by_dst = {}, {}
    for e, (s, d, _, _) in enumerate(edges):
        by_src.setdefault(s, []).append(e)
        by_dst.setdefault(d, []).append(e)
    colour = {}
    for first in range(len(edges)):
        e = first
        while e not in colour:
            colour[e] = 0
            s = edges[e][0]
            other = [k for k in by_src[s] if k != e][0]
            colour[other] = 1
            d = edges[other][1]
            e = [k for k in by_dst[d] if k != other][0]
    pairs = ([], [])
    table = np.zeros((512, 4), np.int32)
    for e, (s, d, half, turned) in enumerate(edges):
        k = colour[e]
        pairs[k].append((s, d))
        table[d, 2 * k] = turned
        if k == 0:
            table[d, 1] = half
    for mp in range(16):
        for h in range(2):
            own, other = number(mp, h, mp), number(mp, 1 - h, mp)
            pairs[1].append((own, other))
            table[own] = (0, h, 0, 1)
    return pairs, table


def around(x, axis, by):
    n = lax.axis_size(axis)
    return lax.ppermute(x, axis, [((i + by) % n, i) for i in range(n)])


def flipped(x, axis, bit=1):
    n = lax.axis_size(axis)
    return lax.ppermute(x, axis, [(i, i ^ bit) for i in range(n)])


def products(where_ref, f0, f1, f2, f3, c1, ct, keep, send):
    x, z, core, count = where_ref[0], where_ref[1], where_ref[2], where_ref[3]
    dims = (((0,), (0,)), ((), ()))
    r = lax.broadcasted_iota(jnp.int32, (HALF, HALF), 0)
    c = lax.broadcasted_iota(jnp.int32, (HALF, HALF), 1)
    extra_row = lax.broadcasted_iota(jnp.int32, (EXTRA, HALF), 0)
    counted = jnp.where(extra_row == 1, count.astype(jnp.float32), 0.0)
    for o, f in enumerate((f0, f1, f2, f3)):
        a = lax.rem(x + o, 4)

        def put(zeta, q0, q1):
            slot = zeta * 4 + a
            keep[slot, :HALF] = jnp.where(core == 0, q0, q1)
            send[slot, :HALF] = jnp.where(core == 0, q1, q0)
            keep[slot, HALF:] = counted
            send[slot, HALF:] = counted

        lhs = f[...]
        for k, block in enumerate((f0, c1, ct)):
            p = lax.dot_general(lhs, block[...], dims, preferred_element_type=jnp.float32)
            p00, p01, p10, p11 = p[:HALF, :HALF], p[:HALF, HALF:], p[HALF:, :HALF], p[HALF:, HALF:]
            if k == 0:
                reach = jnp.where(a > x, HALF, jnp.where(a == x, 0, -HALF))
                same = r - c <= reach
                put(z, jnp.where(same, p00, p01), jnp.where(same, p11, p10))
                middle = jnp.sum(jnp.where((r == c) & (a == x), p01, 0.0), axis=0, keepdims=True)
                middle = jnp.where(extra_row == 0, middle, counted)
                keep[z * 4 + a, HALF:] = middle
                send[z * 4 + a, HALF:] = middle
            elif k == 1:
                same = lax.rem(z, 2) == 1
                put(z ^ 1, jnp.where(same, p00, p01), jnp.where(same, p11, p10))
            else:
                put(z ^ 2, p00, p10)
                put(z ^ 3, p01, p11)


def all_products(where, rows, c1, ct):
    shape = jax.ShapeDtypeStruct((16, HALF + EXTRA, HALF), jnp.float32)
    vmem = pl.BlockSpec(memory_space=pltpu.VMEM)
    return pl.pallas_call(
        products,
        out_shape=(shape, shape),
        in_specs=[pl.BlockSpec(memory_space=pltpu.SMEM)] + [vmem] * 6,
        out_specs=(vmem, vmem),
        compiler_params=pltpu.CompilerParams(vmem_limit_bytes=16 << 20),
        cost_estimate=pl.CostEstimate(flops=2 * 1024 * 1024 * 768, bytes_accessed=5 << 20, transcendentals=0),
        name="products",
    )(where, *rows, c1, ct)


def scale_of(code):
    return jnp.exp2(code * (1.0 / 256.0))


def encode(keep, got, out):
    row = lax.broadcasted_iota(jnp.int32, (PACK, HALF), 0)

    def one(slot, carry):
        v = keep[slot, :HALF] + got[slot, :HALF]
        extra = keep[slot, HALF:] + got[slot, HALF:]
        middle, count = extra[0:1], extra[1:2]
        most = jnp.maximum(jnp.max(jnp.abs(v), axis=0, keepdims=True), jnp.abs(middle))
        code = jnp.ceil(jnp.log2(jnp.maximum(most, 1e-37)) * 256.0)
        rate = LEVELS / scale_of(code)
        tail = jnp.where(row == 0, middle * rate, jnp.where(row == 1, code, jnp.where(row == 2, count, 0.0)))
        out[slot, :HALF] = whole(v * rate)
        out[slot, HALF:] = whole(tail)
        return carry

    lax.fori_loop(0, 16, one, 0)


def whole(v):
    return jnp.clip(jnp.round(v), -LEVELS, LEVELS).astype(jnp.int32).astype(jnp.int16)


def decode(coded, quad, extra, message):
    row = lax.broadcasted_iota(jnp.int32, (EXTRA, HALF), 0)

    def one(slot, carry):
        total, rest = carry
        tail = coded[slot, HALF:].astype(jnp.int32).astype(jnp.float32)
        scale = scale_of(tail[1:2]) * (1.0 / LEVELS)
        total = total + coded[slot, :HALF].astype(jnp.int32).astype(jnp.float32) * scale
        rest = rest + jnp.where(row == 0, tail[0:1] * scale, jnp.where(row == 1, tail[2:3], 0.0))
        return total, rest

    start = jnp.zeros((HALF, HALF), jnp.float32), jnp.zeros((EXTRA, HALF), jnp.float32)
    total, extra[...] = lax.fori_loop(0, 16, one, start)
    quad[...] = total
    most = jnp.max(jnp.abs(total), axis=0, keepdims=True)
    code = jnp.ceil(jnp.log2(jnp.maximum(most, 1e-37)) * 256.0)
    message[:HALF] = whole(total * (LEVELS / scale_of(code)))
    message[HALF:] = whole(jnp.broadcast_to(code, (PACK, HALF)))


def opened(message):
    scale = scale_of(message[HALF:].astype(jnp.int32).astype(jnp.float32)[:1]) * (1.0 / LEVELS)
    return message[:HALF].astype(jnp.int32).astype(jnp.float32) * scale


def encoded(keep, got):
    return pl.pallas_call(
        encode,
        out_shape=jax.ShapeDtypeStruct((16, HALF + PACK, HALF), jnp.int16),
        in_specs=[VMEM] * 2,
        out_specs=VMEM,
        compiler_params=pltpu.CompilerParams(vmem_limit_bytes=8 << 20),
        cost_estimate=pl.CostEstimate(flops=2 << 20, bytes_accessed=3 << 20, transcendentals=0),
        name="encode",
    )(keep, got)


def decoded(coded):
    return pl.pallas_call(
        decode,
        out_shape=(
            jax.ShapeDtypeStruct((HALF, HALF), jnp.float32),
            jax.ShapeDtypeStruct((EXTRA, HALF), jnp.float32),
            jax.ShapeDtypeStruct((HALF + PACK, HALF), jnp.int16),
        ),
        in_specs=[VMEM],
        out_specs=(VMEM, VMEM, VMEM),
        compiler_params=pltpu.CompilerParams(vmem_limit_bytes=8 << 20),
        cost_estimate=pl.CostEstimate(flops=2 << 20, bytes_accessed=1 << 20, transcendentals=0),
        name="decode",
    )(coded)


def assemble(how, quad, extra, r1, r2, out):
    turn1, half1, turn2, diagonal = how[0] == 1, how[1], how[2] == 1, how[3] == 1
    r = lax.broadcasted_iota(jnp.int32, (HALF, HALF), 0)
    c = lax.broadcasted_iota(jnp.int32, (HALF, HALF), 1)
    m, got1, got2 = quad[...], opened(r1), opened(r2)
    turned2 = got2.T
    own = jnp.where(r <= c, m, m.T)
    cross = jnp.where(r > c, m, jnp.where(r == c, extra[0:1], turned2))
    q1 = jnp.where(diagonal, own, jnp.where(turn1, got1.T, got1))
    q2 = jnp.where(diagonal, cross, jnp.where(turn2, turned2, got2))
    total = extra[1:2]
    out[:, :HALF] = jnp.where(half1 == 0, q1, q2) / total
    out[:, HALF:] = jnp.where(half1 == 0, q2, q1) / total


def assembled(how, quad, extra, r1, r2):
    vmem = pl.BlockSpec(memory_space=pltpu.VMEM)
    return pl.pallas_call(
        assemble,
        out_shape=jax.ShapeDtypeStruct((HALF, 2 * HALF), jnp.float32),
        in_specs=[pl.BlockSpec(memory_space=pltpu.SMEM)] + [vmem] * 4,
        out_specs=vmem,
        compiler_params=pltpu.CompilerParams(vmem_limit_bytes=4 << 20),
        cost_estimate=pl.CostEstimate(flops=1 << 20, bytes_accessed=1 << 19, transcendentals=0),
        name="assemble",
    )(how, quad, extra, r1, r2)


def activated(window_of, code, weights, bias):
    v = bias
    for lag in range(weights.shape[0]):
        v = v + jnp.where(code >= lag, weights[lag : lag + 1] * window_of(lag), 0.0)
    return jnp.where(code >= 0, v * (1.0 / (1.0 + jnp.exp(-v))), 0.0)


def codes(group, doc_start, counts):
    token = group * HALF + lax.broadcasted_iota(jnp.int32, (1, HALF), 1)
    place = lax.axis_index(SEQ) * (8 * HALF) + token
    age = jnp.minimum(place - doc_start[group : group + 1, :], 3)
    code = jnp.where(token < counts[0], age, -1).astype(jnp.float32)
    column = jnp.broadcast_to(code, (HALF, HALF)).T
    return jnp.concatenate([column, column], axis=1)


def conv_body(counts, inputs, weights, bias, doc_start, out, lead, x_in, w_in, b_in, d_in, sems):
    moves = [
        pltpu.make_async_copy(src, dst, sems.at[k])
        for k, (src, dst) in enumerate(((inputs, x_in), (weights, w_in), (bias, b_in), (doc_start, d_in)))
    ]
    for move in moves:
        move.start()
    for move in moves:
        move.wait()
    w = w_in[...].astype(jnp.float32)
    b = b_in[...].reshape(1, 2 * HALF).astype(jnp.float32)
    lead[:16] = x_in[:16, :].astype(jnp.float32)
    lead[16:32] = codes(0, d_in, counts)[:16]
    lead[32:36] = w
    lead[36:37] = b
    for group in range(8):
        base = group * HALF
        code = codes(group, d_in, counts)
        if group:
            wide = x_in[base - 16 : base + HALF, :].astype(jnp.float32)
        else:
            wide = jnp.concatenate([jnp.zeros((16, 2 * HALF), jnp.float32), x_in[:HALF, :].astype(jnp.float32)], axis=0)
        value = activated(lambda lag: wide[16 - lag : 16 - lag + HALF], code, w, b)
        out[base : base + HALF, :] = value.astype(jnp.bfloat16)


def head_body(main, lead, prior, own):
    wide = jnp.concatenate([prior[...].astype(jnp.float32), lead[:16]], axis=0)
    value = activated(lambda lag: wide[8 - lag : 24 - lag], lead[16:32], lead[32:36], lead[36:37])
    own[:16, :] = value.astype(jnp.bfloat16)
    own[16:, :] = main[16:, :]


def conv_main(counts, inputs, weights, bias, doc_start):
    fixed = [pltpu.with_memory_space_constraint(v, pltpu.HBM) for v in (inputs, weights, bias, doc_start)]
    return pl.pallas_call(
        conv_body,
        out_shape=(
            jax.ShapeDtypeStruct(inputs.shape, jnp.bfloat16),
            jax.ShapeDtypeStruct((40, inputs.shape[1]), jnp.float32),
        ),
        in_specs=[SMEM] + [pl.BlockSpec(memory_space=pltpu.HBM)] * 4,
        out_specs=(VMEM, VMEM),
        scratch_shapes=[pltpu.VMEM(v.shape, v.dtype) for v in (inputs, weights, bias, doc_start)]
        + [pltpu.SemaphoreType.DMA((4,))],
        compiler_params=pltpu.CompilerParams(vmem_limit_bytes=8 << 20),
        cost_estimate=pl.CostEstimate(flops=8 << 20, bytes_accessed=1 << 20, transcendentals=1 << 19),
        name="conv_main",
    )(counts, *fixed)


def conv_head(main, lead, prior):
    return pl.pallas_call(
        head_body,
        out_shape=jax.ShapeDtypeStruct(main.shape, jnp.bfloat16),
        in_specs=[VMEM] * 3,
        out_specs=VMEM,
        compiler_params=pltpu.CompilerParams(vmem_limit_bytes=8 << 20),
        cost_estimate=pl.CostEstimate(flops=1 << 20, bytes_accessed=1 << 20, transcendentals=0),
        name="conv_head",
    )(main, lead, prior)


def on_device(inputs, conv_weight, conv_bias, doc_start, counts):
    pairs, table = delivery()
    length, _ = inputs.shape
    core, z, x = lax.axis_index(CORE), lax.axis_index(ZL), lax.axis_index(X)
    count = counts[0]

    shards = lax.axis_size(SEQ)
    prior = lax.ppermute(inputs[length - 8 :], SEQ, [(i, i + 1) for i in range(shards - 1)])
    starts = doc_start.reshape(8, HALF)
    main, lead = conv_main(counts, inputs, conv_weight, conv_bias, starts)
    own = conv_head(main, lead, prior)

    ct = lax.ppermute(own, ZL, [(TAU[i], i) for i in range(4)])
    f1 = around(own, X, 1)
    f3 = around(own, X, 3)
    f2 = around(own, X, 2)
    c1 = flipped(own, ZL)

    where = jnp.stack([x, z, core, count]).astype(jnp.int32)
    keep, send = all_products(where, (own, f1, f2, f3), c1, ct)
    coded = encoded(keep, flipped(send, CORE))
    quad, extra, message = decoded(lax.all_to_all(coded, CHIPS, split_axis=0, concat_axis=0, tiled=True))

    r1 = lax.ppermute(message, AXES, pairs[0])
    r2 = lax.ppermute(message, AXES, pairs[1])
    how = lax.dynamic_index_in_dim(jnp.asarray(table), lax.axis_index(AXES), keepdims=False)
    return assembled(how, quad, extra, r1, r2)


def solution(mesh):
    torus = Mesh(mesh.devices.reshape(SIZES), AXES)
    mp = (ZL, X)
    placed = (P(SEQ, mp), P(None, mp), P(mp), P(SEQ), P(SEQ))

    return jax.shard_map(on_device, mesh=torus, in_specs=placed, out_specs=P(SEQ, mp), check_vma=False)
```

```python
import functools

import jax
import jax.numpy as jnp
import numpy as np
from jax import lax
from jax.experimental import pallas as pl
from jax.experimental.pallas import tpu as pltpu
from jax.sharding import Mesh
from jax.sharding import PartitionSpec as P


ZH, YW, YA, CORE, ZL, X = AXES = ("zh", "yw", "ya", "core", "zl", "x")
SIZES = (2, 2, 4, 2, 4, 4)
SEQ = (ZH, YW, YA, CORE)
CHIPS = (ZH, YW, YA)
TAU = (3, 2, 0, 1)
EARLY = ((0, "own"), (0, "far"), (2, "own"), (2, "far"))
LATE = ((1, "own"), (1, "far"), (1, "near"), (3, "own"), (3, "far"), (3, "near"), (0, "near"), (2, "near"))
HALF = 128
EXTRA = 8
PACK = 8
LEVELS = 32767.0
VMEM = pl.BlockSpec(memory_space=pltpu.VMEM)
SMEM = pl.BlockSpec(memory_space=pltpu.SMEM)


def delivery():
    def number(seq_chip, core, mp):
        return (seq_chip * 2 + core) * 16 + mp

    edges = []
    for seq_chip in range(16):
        for h in range(2):
            for mp in range(16):
                zeta, a = divmod(seq_chip, 4)
                z, x = divmod(mp, 4)
                row = 4 * z + a
                if zeta == z:
                    col, hc = 4 * z + x, (h if a >= x else 1 - h)
                elif zeta == z ^ 1:
                    col, hc = 4 * (z ^ 1) + x, (h if z % 2 else 1 - h)
                else:
                    col, hc = 4 * TAU[z] + x, (0 if zeta == z ^ 2 else 1)
                src = number(seq_chip, h, mp)
                if row == col:
                    continue
                edges.append((src, number(row, h, col), hc, 0))
                edges.append((src, number(col, hc, row), h, 1))
    by_src, by_dst = {}, {}
    for e, (s, d, _, _) in enumerate(edges):
        by_src.setdefault(s, []).append(e)
        by_dst.setdefault(d, []).append(e)
    colour = {}
    for first in range(len(edges)):
        e = first
        while e not in colour:
            colour[e] = 0
            s = edges[e][0]
            other = [k for k in by_src[s] if k != e][0]
            colour[other] = 1
            d = edges[other][1]
            e = [k for k in by_dst[d] if k != other][0]
    pairs = ([], [])
    table = np.zeros((512, 4), np.int32)
    for e, (s, d, half, turned) in enumerate(edges):
        k = colour[e]
        pairs[k].append((s, d))
        table[d, 2 * k] = turned
        if k == 0:
            table[d, 1] = half
    for mp in range(16):
        for h in range(2):
            own, other = number(mp, h, mp), number(mp, 1 - h, mp)
            pairs[1].append((own, other))
            table[own] = (0, h, 0, 1)
    return pairs, table


def around(x, axis, by):
    n = lax.axis_size(axis)
    return lax.ppermute(x, axis, [((i + by) % n, i) for i in range(n)])


def flipped(x, axis, bit=1):
    n = lax.axis_size(axis)
    return lax.ppermute(x, axis, [(i, i ^ bit) for i in range(n)])


def products(late, where_ref, *refs):
    x, z, core, count = where_ref[0], where_ref[1], where_ref[2], where_ref[3]
    keep, send = refs[-2:]
    rows = dict(zip((0, 2, 1, 3) if late else (0, 2), refs))
    cols = {"own": refs[0], "far": refs[4], "near": refs[5]} if late else {"own": refs[0], "far": refs[2]}
    dims = (((0,), (0,)), ((), ()))
    r = lax.broadcasted_iota(jnp.int32, (HALF, HALF), 0)
    c = lax.broadcasted_iota(jnp.int32, (HALF, HALF), 1)
    extra_row = lax.broadcasted_iota(jnp.int32, (EXTRA, HALF), 0)
    counted = jnp.where(extra_row == 1, count.astype(jnp.float32), 0.0)
    found = {}
    for o, kind in LATE if late else EARLY:
        a = lax.rem(x + o, 4)
        p = lax.dot_general(rows[o][...], cols[kind][...], dims, preferred_element_type=jnp.float32)
        p00, p01, p10, p11 = p[:HALF, :HALF], p[:HALF, HALF:], p[HALF:, :HALF], p[HALF:, HALF:]
        extra = counted
        if kind == "own":
            same = r <= c if o == 0 else a > x
            found[0, o] = jnp.where(same, p00, p01), jnp.where(same, p11, p10)
            if o == 0:
                middle = jnp.sum(jnp.where(r == c, p01, 0.0), axis=0, keepdims=True)
                extra = jnp.where(extra_row == 0, middle, counted)
        elif kind == "near":
            same = lax.rem(z, 2) == 1
            found[1, o] = jnp.where(same, p00, p01), jnp.where(same, p11, p10)
        else:
            found[2, o] = p00, p10
            found[3, o] = p01, p11
        for k in {"own": (0,), "near": (1,), "far": (2, 3)}[kind]:
            at = slots(late).index((k, o))
            q0, q1 = found[k, o]
            keep[at, :HALF] = jnp.where(core == 0, q0, q1)
            send[at, :HALF] = jnp.where(core == 0, q1, q0)
            keep[at, HALF:] = extra
            send[at, HALF:] = extra


def slots(late):
    kinds = {"own": (0,), "near": (1,), "far": (2, 3)}
    return [(k, o) for o, kind in (LATE if late else EARLY) for k in kinds[kind]]


def multiplied(late, where, *blocks):
    shape = jax.ShapeDtypeStruct((len(slots(late)), HALF + EXTRA, HALF), jnp.float32)
    return pl.pallas_call(
        functools.partial(products, late),
        out_shape=(shape, shape),
        in_specs=[SMEM] + [VMEM] * len(blocks),
        out_specs=(VMEM, VMEM),
        compiler_params=pltpu.CompilerParams(vmem_limit_bytes=16 << 20),
        cost_estimate=pl.CostEstimate(
            flops=(1 << 27) * len(LATE if late else EARLY), bytes_accessed=5 << 20, transcendentals=0
        ),
        name="products_late" if late else "products_early",
    )(where, *blocks)


def scale_of(code):
    return jnp.exp2(code * (1.0 / 256.0))


def encode(late, where_ref, keep, got, *refs):
    row = lax.broadcasted_iota(jnp.int32, (PACK, HALF), 0)
    out = refs[-1]
    for at, (k, o) in enumerate(slots(late)):
        v = keep[at, :HALF] + got[at, :HALF]
        extra = keep[at, HALF:] + got[at, HALF:]
        middle, count = extra[0:1], extra[1:2]
        most = jnp.maximum(jnp.max(jnp.abs(v), axis=0, keepdims=True), jnp.abs(middle))
        code = jnp.ceil(jnp.log2(jnp.maximum(most, 1e-37)) * 256.0)
        rate = LEVELS / scale_of(code)
        tail = jnp.where(row == 0, middle * rate, jnp.where(row == 1, code, jnp.where(row == 2, count, 0.0)))
        slot = place(where_ref, k, o) if late else at
        out[slot, :HALF] = whole(v * rate)
        out[slot, HALF:] = whole(tail)
    if late:
        for at, (k, o) in enumerate(slots(False)):
            out[place(where_ref, k, o)] = refs[0][at]


def place(where_ref, k, o):
    return (where_ref[1] ^ k) * 4 + lax.rem(where_ref[0] + o, 4)


def whole(v):
    return jnp.clip(jnp.round(v), -LEVELS, LEVELS).astype(jnp.int32).astype(jnp.int16)


def decode(coded, quad, extra, message):
    row = lax.broadcasted_iota(jnp.int32, (EXTRA, HALF), 0)

    def one(slot, carry):
        total, rest = carry
        tail = coded[slot, HALF:].astype(jnp.int32).astype(jnp.float32)
        scale = scale_of(tail[1:2]) * (1.0 / LEVELS)
        total = total + coded[slot, :HALF].astype(jnp.int32).astype(jnp.float32) * scale
        rest = rest + jnp.where(row == 0, tail[0:1] * scale, jnp.where(row == 1, tail[2:3], 0.0))
        return total, rest

    start = jnp.zeros((HALF, HALF), jnp.float32), jnp.zeros((EXTRA, HALF), jnp.float32)
    total, extra[...] = lax.fori_loop(0, 16, one, start)
    quad[...] = total
    most = jnp.max(jnp.abs(total), axis=0, keepdims=True)
    code = jnp.ceil(jnp.log2(jnp.maximum(most, 1e-37)) * 256.0)
    message[:HALF] = whole(total * (LEVELS / scale_of(code)))
    message[HALF:] = whole(jnp.broadcast_to(code, (PACK, HALF)))


def opened(message):
    scale = scale_of(message[HALF:].astype(jnp.int32).astype(jnp.float32)[:1]) * (1.0 / LEVELS)
    return message[:HALF].astype(jnp.int32).astype(jnp.float32) * scale


def encoded(late, where, *parts):
    count = 16 if late else len(slots(False))
    return pl.pallas_call(
        functools.partial(encode, late),
        out_shape=jax.ShapeDtypeStruct((count, HALF + PACK, HALF), jnp.int16),
        in_specs=[SMEM] + [VMEM] * len(parts),
        out_specs=VMEM,
        compiler_params=pltpu.CompilerParams(vmem_limit_bytes=8 << 20),
        cost_estimate=pl.CostEstimate(flops=2 << 20, bytes_accessed=3 << 20, transcendentals=0),
        name="encode_late" if late else "encode_early",
    )(where, *parts)


def decoded(coded):
    return pl.pallas_call(
        decode,
        out_shape=(
            jax.ShapeDtypeStruct((HALF, HALF), jnp.float32),
            jax.ShapeDtypeStruct((EXTRA, HALF), jnp.float32),
            jax.ShapeDtypeStruct((HALF + PACK, HALF), jnp.int16),
        ),
        in_specs=[VMEM],
        out_specs=(VMEM, VMEM, VMEM),
        compiler_params=pltpu.CompilerParams(vmem_limit_bytes=8 << 20),
        cost_estimate=pl.CostEstimate(flops=2 << 20, bytes_accessed=1 << 20, transcendentals=0),
        name="decode",
    )(coded)


def assemble(how, quad, extra, r1, r2, out):
    turn1, half1, turn2, diagonal = how[0] == 1, how[1], how[2] == 1, how[3] == 1
    r = lax.broadcasted_iota(jnp.int32, (HALF, HALF), 0)
    c = lax.broadcasted_iota(jnp.int32, (HALF, HALF), 1)
    m, got1, got2 = quad[...], opened(r1), opened(r2)
    turned2 = got2.T
    own = jnp.where(r <= c, m, m.T)
    cross = jnp.where(r > c, m, jnp.where(r == c, extra[0:1], turned2))
    q1 = jnp.where(diagonal, own, jnp.where(turn1, got1.T, got1))
    q2 = jnp.where(diagonal, cross, jnp.where(turn2, turned2, got2))
    total = extra[1:2]
    out[:, :HALF] = jnp.where(half1 == 0, q1, q2) / total
    out[:, HALF:] = jnp.where(half1 == 0, q2, q1) / total


def assembled(how, quad, extra, r1, r2):
    vmem = pl.BlockSpec(memory_space=pltpu.VMEM)
    return pl.pallas_call(
        assemble,
        out_shape=jax.ShapeDtypeStruct((HALF, 2 * HALF), jnp.float32),
        in_specs=[pl.BlockSpec(memory_space=pltpu.SMEM)] + [vmem] * 4,
        out_specs=vmem,
        compiler_params=pltpu.CompilerParams(vmem_limit_bytes=4 << 20),
        cost_estimate=pl.CostEstimate(flops=1 << 20, bytes_accessed=1 << 19, transcendentals=0),
        name="assemble",
    )(how, quad, extra, r1, r2)


def activated(window_of, code, weights, bias):
    v = bias
    for lag in range(weights.shape[0]):
        v = v + jnp.where(code >= lag, weights[lag : lag + 1] * window_of(lag), 0.0)
    return jnp.where(code >= 0, v * (1.0 / (1.0 + jnp.exp(-v))), 0.0)


def codes(group, doc_start, counts):
    token = group * HALF + lax.broadcasted_iota(jnp.int32, (1, HALF), 1)
    place = lax.axis_index(SEQ) * (8 * HALF) + token
    age = jnp.minimum(place - doc_start[group : group + 1, :], 3)
    code = jnp.where(token < counts[0], age, -1).astype(jnp.float32)
    column = jnp.broadcast_to(code, (HALF, HALF)).T
    return jnp.concatenate([column, column], axis=1)


def conv_body(counts, inputs, weights, bias, doc_start, out, lead, x_in, w_in, b_in, d_in, sems):
    moves = [
        pltpu.make_async_copy(src, dst, sems.at[k])
        for k, (src, dst) in enumerate(((inputs, x_in), (weights, w_in), (bias, b_in), (doc_start, d_in)))
    ]
    for move in moves:
        move.start()
    for move in moves:
        move.wait()
    w = w_in[...].astype(jnp.float32)
    b = b_in[...].reshape(1, 2 * HALF).astype(jnp.float32)
    lead[:16] = x_in[:16, :].astype(jnp.float32)
    lead[16:32] = codes(0, d_in, counts)[:16]
    lead[32:36] = w
    lead[36:37] = b
    for group in range(8):
        base = group * HALF
        code = codes(group, d_in, counts)
        if group:
            wide = x_in[base - 16 : base + HALF, :].astype(jnp.float32)
        else:
            wide = jnp.concatenate([jnp.zeros((16, 2 * HALF), jnp.float32), x_in[:HALF, :].astype(jnp.float32)], axis=0)
        value = activated(lambda lag: wide[16 - lag : 16 - lag + HALF], code, w, b)
        out[base : base + HALF, :] = value.astype(jnp.bfloat16)


def head_body(main, lead, prior, own):
    wide = jnp.concatenate([prior[...].astype(jnp.float32), lead[:16]], axis=0)
    value = activated(lambda lag: wide[8 - lag : 24 - lag], lead[16:32], lead[32:36], lead[36:37])
    own[:16, :] = value.astype(jnp.bfloat16)
    own[16:, :] = main[16:, :]


def conv_main(counts, inputs, weights, bias, doc_start):
    fixed = [pltpu.with_memory_space_constraint(v, pltpu.HBM) for v in (inputs, weights, bias, doc_start)]
    return pl.pallas_call(
        conv_body,
        out_shape=(
            jax.ShapeDtypeStruct(inputs.shape, jnp.bfloat16),
            jax.ShapeDtypeStruct((40, inputs.shape[1]), jnp.float32),
        ),
        in_specs=[SMEM] + [pl.BlockSpec(memory_space=pltpu.HBM)] * 4,
        out_specs=(VMEM, VMEM),
        scratch_shapes=[pltpu.VMEM(v.shape, v.dtype) for v in (inputs, weights, bias, doc_start)]
        + [pltpu.SemaphoreType.DMA((4,))],
        compiler_params=pltpu.CompilerParams(vmem_limit_bytes=8 << 20),
        cost_estimate=pl.CostEstimate(flops=8 << 20, bytes_accessed=1 << 20, transcendentals=1 << 19),
        name="conv_main",
    )(counts, *fixed)


def conv_head(main, lead, prior):
    return pl.pallas_call(
        head_body,
        out_shape=jax.ShapeDtypeStruct(main.shape, jnp.bfloat16),
        in_specs=[VMEM] * 3,
        out_specs=VMEM,
        compiler_params=pltpu.CompilerParams(vmem_limit_bytes=8 << 20),
        cost_estimate=pl.CostEstimate(flops=1 << 20, bytes_accessed=1 << 20, transcendentals=0),
        name="conv_head",
    )(main, lead, prior)


def on_device(inputs, conv_weight, conv_bias, doc_start, counts):
    pairs, table = delivery()
    length, _ = inputs.shape
    core, z, x = lax.axis_index(CORE), lax.axis_index(ZL), lax.axis_index(X)
    count = counts[0]

    shards = lax.axis_size(SEQ)
    prior = lax.ppermute(inputs[length - 8 :], SEQ, [(i, i + 1) for i in range(shards - 1)])
    starts = doc_start.reshape(8, HALF)
    main, lead = conv_main(counts, inputs, conv_weight, conv_bias, starts)
    own = conv_head(main, lead, prior)

    ct = lax.ppermute(own, ZL, [(TAU[i], i) for i in range(4)])
    f1 = around(own, X, 1)
    f3 = around(own, X, 3)
    f2 = around(own, X, 2)
    c1 = flipped(own, ZL)

    where = jnp.stack([x, z, core, count]).astype(jnp.int32)
    keep, send = multiplied(False, where, own, f2, ct)
    got = flipped(send, CORE)
    first = encoded(False, where, keep, got)
    keep, send = multiplied(True, where, own, f2, f1, f3, ct, c1)
    coded = encoded(True, where, keep, flipped(send, CORE), first)
    quad, extra, message = decoded(lax.all_to_all(coded, CHIPS, split_axis=0, concat_axis=0, tiled=True))

    r1 = lax.ppermute(message, AXES, pairs[0])
    r2 = lax.ppermute(message, AXES, pairs[1])
    how = lax.dynamic_index_in_dim(jnp.asarray(table), lax.axis_index(AXES), keepdims=False)
    return assembled(how, quad, extra, r1, r2)


def solution(mesh):
    torus = Mesh(mesh.devices.reshape(SIZES), AXES)
    mp = (ZL, X)
    placed = (P(SEQ, mp), P(None, mp), P(mp), P(SEQ), P(SEQ))

    return jax.shard_map(on_device, mesh=torus, in_specs=placed, out_specs=P(SEQ, mp), check_vma=False)
```

```python
import functools

import jax
import jax.numpy as jnp
import numpy as np
from jax import lax
from jax.experimental import pallas as pl
from jax.experimental.pallas import tpu as pltpu
from jax.sharding import Mesh
from jax.sharding import PartitionSpec as P


ZH, YW, YA, CORE, ZL, X = AXES = ("zh", "yw", "ya", "core", "zl", "x")
SIZES = (2, 2, 4, 2, 4, 4)
SEQ = (ZH, YW, YA, CORE)
CHIPS = (ZH, YW, YA)
TAU = (3, 2, 0, 1)
HOMES = tuple(tuple(4 * (mp // 4 ^ k) + a for k in range(4) for a in range(4)) for mp in range(16))
NEAR_FIRST = False
EARLY = ((0, "own"), (0, "far"), (2, "own"), (2, "far"))
LATE = ((1, "own"), (1, "far"), (1, "near"), (3, "own"), (3, "far"), (3, "near"), (0, "near"), (2, "near"))
HALF = 128
EXTRA = 8
PACK = 8
LEVELS = 32767.0
VMEM = pl.BlockSpec(memory_space=pltpu.VMEM)
SMEM = pl.BlockSpec(memory_space=pltpu.SMEM)


def number(chip, core, mp):
    return (chip * 2 + core) * 16 + mp


def hops(p, q):
    def coordinates(device):
        seq, mp = divmod(device, 16)
        return mp % 4, seq // 2 % 8, seq // 16 * 4 + mp // 4

    return sum(min((i - j) % n, (j - i) % n) for i, j, n in zip(coordinates(p), coordinates(q), (4, 8, 8)))


def delivery():
    edges = []
    for mp, homes in enumerate(HOMES):
        z, x = divmod(mp, 4)
        for content, chip in enumerate(homes):
            kind, a = divmod(content, 4)
            row, col = 4 * z + a, 4 * (z, z ^ 1, TAU[z], TAU[z])[kind] + x
            if row == col:
                continue
            for h in range(2):
                same = (a >= x, z % 2 == 1, h == 0, h == 1)[kind]
                hc = h if same else 1 - h
                src = number(chip, h, mp)
                edges.append((src, number(row, h, col), hc, 0))
                edges.append((src, number(col, hc, row), h, 1))
    by_dst = {}
    for e, (_, d, _, _) in enumerate(edges):
        by_dst.setdefault(d, []).append(e)
    seen, rounds = set(), ([], [])
    for start in range(0, len(edges), 2):
        if start in seen:
            continue
        cycle, e = ([], []), start
        while e not in seen:
            seen.update((e, e ^ 1))
            cycle[0].append(e)
            cycle[1].append(e ^ 1)
            e = sum(by_dst[edges[e ^ 1][1]]) - (e ^ 1)
        weight = [sum(2.0 ** hops(*edges[k][:2]) for k in part) for part in cycle]
        first = 0 if (weight[0] <= weight[1]) == NEAR_FIRST else 1
        rounds[1].extend(cycle[first])
        rounds[0].extend(cycle[1 - first])
    table = np.zeros((512, 4), np.int32)
    for k in range(2):
        for e in rounds[k]:
            _, d, half, turned = edges[e]
            table[d, 2 * k] = turned
            if k == 0:
                table[d, 1] = half
    pairs = tuple([edges[e][:2] for e in part] for part in rounds)
    for mp in range(16):
        for h in range(2):
            own, other = number(mp, h, mp), number(mp, 1 - h, mp)
            pairs[1].append((own, other))
            table[own] = (0, h, 0, 1)
    return pairs, table


def around(x, axis, by):
    n = lax.axis_size(axis)
    return lax.ppermute(x, axis, [((i + by) % n, i) for i in range(n)])


def flipped(x, axis, bit=1):
    n = lax.axis_size(axis)
    return lax.ppermute(x, axis, [(i, i ^ bit) for i in range(n)])


def products(late, where_ref, *refs):
    x, z, core, count = where_ref[0], where_ref[1], where_ref[2], where_ref[3]
    keep, send = refs[-2:]
    rows = dict(zip((0, 2, 1, 3) if late else (0, 2), refs))
    cols = {"own": refs[0], "far": refs[4], "near": refs[5]} if late else {"own": refs[0], "far": refs[2]}
    dims = (((0,), (0,)), ((), ()))
    r = lax.broadcasted_iota(jnp.int32, (HALF, HALF), 0)
    c = lax.broadcasted_iota(jnp.int32, (HALF, HALF), 1)
    extra_row = lax.broadcasted_iota(jnp.int32, (EXTRA, HALF), 0)
    counted = jnp.where(extra_row == 1, count.astype(jnp.float32), 0.0)
    found = {}
    for o, kind in LATE if late else EARLY:
        a = lax.rem(x + o, 4)
        p = lax.dot_general(rows[o][...], cols[kind][...], dims, preferred_element_type=jnp.float32)
        p00, p01, p10, p11 = p[:HALF, :HALF], p[:HALF, HALF:], p[HALF:, :HALF], p[HALF:, HALF:]
        extra = counted
        if kind == "own":
            same = r <= c if o == 0 else a > x
            found[0, o] = jnp.where(same, p00, p01), jnp.where(same, p11, p10)
            if o == 0:
                middle = jnp.sum(jnp.where(r == c, p01, 0.0), axis=0, keepdims=True)
                extra = jnp.where(extra_row == 0, middle, counted)
        elif kind == "near":
            same = lax.rem(z, 2) == 1
            found[1, o] = jnp.where(same, p00, p01), jnp.where(same, p11, p10)
        else:
            found[2, o] = p00, p10
            found[3, o] = p01, p11
        for k in {"own": (0,), "near": (1,), "far": (2, 3)}[kind]:
            at = slots(late).index((k, o))
            q0, q1 = found[k, o]
            keep[at, :HALF] = jnp.where(core == 0, q0, q1)
            send[at, :HALF] = jnp.where(core == 0, q1, q0)
            keep[at, HALF:] = extra
            send[at, HALF:] = extra


def slots(late):
    kinds = {"own": (0,), "near": (1,), "far": (2, 3)}
    return [(k, o) for o, kind in (LATE if late else EARLY) for k in kinds[kind]]


def multiplied(late, where, *blocks):
    shape = jax.ShapeDtypeStruct((len(slots(late)), HALF + EXTRA, HALF), jnp.float32)
    return pl.pallas_call(
        functools.partial(products, late),
        out_shape=(shape, shape),
        in_specs=[SMEM] + [VMEM] * len(blocks),
        out_specs=(VMEM, VMEM),
        compiler_params=pltpu.CompilerParams(vmem_limit_bytes=16 << 20),
        cost_estimate=pl.CostEstimate(
            flops=(1 << 27) * len(LATE if late else EARLY), bytes_accessed=5 << 20, transcendentals=0
        ),
        name="products_late" if late else "products_early",
    )(where, *blocks)


def scale_of(code):
    return jnp.exp2(code * (1.0 / 256.0))


def encode(late, where_ref, keep, got, *refs):
    row = lax.broadcasted_iota(jnp.int32, (PACK, HALF), 0)
    out = refs[-1]
    for at, (k, o) in enumerate(slots(late)):
        v = keep[at, :HALF] + got[at, :HALF]
        extra = keep[at, HALF:] + got[at, HALF:]
        middle, count = extra[0:1], extra[1:2]
        most = jnp.maximum(jnp.max(jnp.abs(v), axis=0, keepdims=True), jnp.abs(middle))
        code = jnp.ceil(jnp.log2(jnp.maximum(most, 1e-37)) * 256.0)
        rate = LEVELS / scale_of(code)
        tail = jnp.where(row == 0, middle * rate, jnp.where(row == 1, code, jnp.where(row == 2, count, 0.0)))
        slot = place(where_ref, k, o) if late else at
        out[slot, :HALF] = whole(v * rate)
        out[slot, HALF:] = whole(tail)
    if late:
        for at, (k, o) in enumerate(slots(False)):
            out[place(where_ref, k, o)] = refs[0][at]


def place(where_ref, k, o):
    return where_ref[4 + 4 * k + lax.rem(where_ref[0] + o, 4)]


def whole(v):
    return jnp.clip(jnp.round(v), -LEVELS, LEVELS).astype(jnp.int32).astype(jnp.int16)


def decode(coded, quad, extra, message):
    row = lax.broadcasted_iota(jnp.int32, (EXTRA, HALF), 0)

    def one(slot, carry):
        total, rest = carry
        tail = coded[slot, HALF:].astype(jnp.int32).astype(jnp.float32)
        scale = scale_of(tail[1:2]) * (1.0 / LEVELS)
        total = total + coded[slot, :HALF].astype(jnp.int32).astype(jnp.float32) * scale
        rest = rest + jnp.where(row == 0, tail[0:1] * scale, jnp.where(row == 1, tail[2:3], 0.0))
        return total, rest

    start = jnp.zeros((HALF, HALF), jnp.float32), jnp.zeros((EXTRA, HALF), jnp.float32)
    total, extra[...] = lax.fori_loop(0, 16, one, start)
    quad[...] = total
    most = jnp.max(jnp.abs(total), axis=0, keepdims=True)
    code = jnp.ceil(jnp.log2(jnp.maximum(most, 1e-37)) * 256.0)
    message[:HALF] = whole(total * (LEVELS / scale_of(code)))
    message[HALF:] = whole(jnp.broadcast_to(code, (PACK, HALF)))


def opened(message):
    scale = scale_of(message[HALF:].astype(jnp.int32).astype(jnp.float32)[:1]) * (1.0 / LEVELS)
    return message[:HALF].astype(jnp.int32).astype(jnp.float32) * scale


def encoded(late, where, *parts):
    count = 16 if late else len(slots(False))
    return pl.pallas_call(
        functools.partial(encode, late),
        out_shape=jax.ShapeDtypeStruct((count, HALF + PACK, HALF), jnp.int16),
        in_specs=[SMEM] + [VMEM] * len(parts),
        out_specs=VMEM,
        compiler_params=pltpu.CompilerParams(vmem_limit_bytes=8 << 20),
        cost_estimate=pl.CostEstimate(flops=2 << 20, bytes_accessed=3 << 20, transcendentals=0),
        name="encode_late" if late else "encode_early",
    )(where, *parts)


def decoded(coded):
    return pl.pallas_call(
        decode,
        out_shape=(
            jax.ShapeDtypeStruct((HALF, HALF), jnp.float32),
            jax.ShapeDtypeStruct((EXTRA, HALF), jnp.float32),
            jax.ShapeDtypeStruct((HALF + PACK, HALF), jnp.int16),
        ),
        in_specs=[VMEM],
        out_specs=(VMEM, VMEM, VMEM),
        compiler_params=pltpu.CompilerParams(vmem_limit_bytes=8 << 20),
        cost_estimate=pl.CostEstimate(flops=2 << 20, bytes_accessed=1 << 20, transcendentals=0),
        name="decode",
    )(coded)


def assemble(how, quad, extra, r1, r2, out):
    turn1, half1, turn2, diagonal = how[0] == 1, how[1], how[2] == 1, how[3] == 1
    r = lax.broadcasted_iota(jnp.int32, (HALF, HALF), 0)
    c = lax.broadcasted_iota(jnp.int32, (HALF, HALF), 1)
    m, got1, got2 = quad[...], opened(r1), opened(r2)
    turned2 = got2.T
    own = jnp.where(r <= c, m, m.T)
    cross = jnp.where(r > c, m, jnp.where(r == c, extra[0:1], turned2))
    q1 = jnp.where(diagonal, own, jnp.where(turn1, got1.T, got1))
    q2 = jnp.where(diagonal, cross, jnp.where(turn2, turned2, got2))
    total = extra[1:2]
    out[:, :HALF] = jnp.where(half1 == 0, q1, q2) / total
    out[:, HALF:] = jnp.where(half1 == 0, q2, q1) / total


def assembled(how, quad, extra, r1, r2):
    vmem = pl.BlockSpec(memory_space=pltpu.VMEM)
    return pl.pallas_call(
        assemble,
        out_shape=jax.ShapeDtypeStruct((HALF, 2 * HALF), jnp.float32),
        in_specs=[pl.BlockSpec(memory_space=pltpu.SMEM)] + [vmem] * 4,
        out_specs=vmem,
        compiler_params=pltpu.CompilerParams(vmem_limit_bytes=4 << 20),
        cost_estimate=pl.CostEstimate(flops=1 << 20, bytes_accessed=1 << 19, transcendentals=0),
        name="assemble",
    )(how, quad, extra, r1, r2)


def activated(window_of, code, weights, bias):
    v = bias
    for lag in range(weights.shape[0]):
        v = v + jnp.where(code >= lag, weights[lag : lag + 1] * window_of(lag), 0.0)
    return jnp.where(code >= 0, v * (1.0 / (1.0 + jnp.exp(-v))), 0.0)


def codes(group, doc_start, counts):
    token = group * HALF + lax.broadcasted_iota(jnp.int32, (1, HALF), 1)
    place = lax.axis_index(SEQ) * (8 * HALF) + token
    age = jnp.minimum(place - doc_start[group : group + 1, :], 3)
    code = jnp.where(token < counts[0], age, -1).astype(jnp.float32)
    column = jnp.broadcast_to(code, (HALF, HALF)).T
    return jnp.concatenate([column, column], axis=1)


def conv_body(counts, inputs, weights, bias, doc_start, out, lead, x_in, w_in, b_in, d_in, sems):
    moves = [
        pltpu.make_async_copy(src, dst, sems.at[k])
        for k, (src, dst) in enumerate(((inputs, x_in), (weights, w_in), (bias, b_in), (doc_start, d_in)))
    ]
    for move in moves:
        move.start()
    for move in moves:
        move.wait()
    w = w_in[...].astype(jnp.float32)
    b = b_in[...].reshape(1, 2 * HALF).astype(jnp.float32)
    lead[:16] = x_in[:16, :].astype(jnp.float32)
    lead[16:32] = codes(0, d_in, counts)[:16]
    lead[32:36] = w
    lead[36:37] = b
    for group in range(8):
        base = group * HALF
        code = codes(group, d_in, counts)
        if group:
            wide = x_in[base - 16 : base + HALF, :].astype(jnp.float32)
        else:
            wide = jnp.concatenate([jnp.zeros((16, 2 * HALF), jnp.float32), x_in[:HALF, :].astype(jnp.float32)], axis=0)
        value = activated(lambda lag: wide[16 - lag : 16 - lag + HALF], code, w, b)
        out[base : base + HALF, :] = value.astype(jnp.bfloat16)


def head_body(main, lead, prior, own):
    wide = jnp.concatenate([prior[...].astype(jnp.float32), lead[:16]], axis=0)
    value = activated(lambda lag: wide[8 - lag : 24 - lag], lead[16:32], lead[32:36], lead[36:37])
    own[:16, :] = value.astype(jnp.bfloat16)
    own[16:, :] = main[16:, :]


def conv_main(counts, inputs, weights, bias, doc_start):
    fixed = [pltpu.with_memory_space_constraint(v, pltpu.HBM) for v in (inputs, weights, bias, doc_start)]
    return pl.pallas_call(
        conv_body,
        out_shape=(
            jax.ShapeDtypeStruct(inputs.shape, jnp.bfloat16),
            jax.ShapeDtypeStruct((40, inputs.shape[1]), jnp.float32),
        ),
        in_specs=[SMEM] + [pl.BlockSpec(memory_space=pltpu.HBM)] * 4,
        out_specs=(VMEM, VMEM),
        scratch_shapes=[pltpu.VMEM(v.shape, v.dtype) for v in (inputs, weights, bias, doc_start)]
        + [pltpu.SemaphoreType.DMA((4,))],
        compiler_params=pltpu.CompilerParams(vmem_limit_bytes=8 << 20),
        cost_estimate=pl.CostEstimate(flops=8 << 20, bytes_accessed=1 << 20, transcendentals=1 << 19),
        name="conv_main",
    )(counts, *fixed)


def conv_head(main, lead, prior):
    return pl.pallas_call(
        head_body,
        out_shape=jax.ShapeDtypeStruct(main.shape, jnp.bfloat16),
        in_specs=[VMEM] * 3,
        out_specs=VMEM,
        compiler_params=pltpu.CompilerParams(vmem_limit_bytes=8 << 20),
        cost_estimate=pl.CostEstimate(flops=1 << 20, bytes_accessed=1 << 20, transcendentals=0),
        name="conv_head",
    )(main, lead, prior)


def on_device(inputs, conv_weight, conv_bias, doc_start, counts):
    pairs, table = delivery()
    length, _ = inputs.shape
    core, z, x = lax.axis_index(CORE), lax.axis_index(ZL), lax.axis_index(X)
    count = counts[0]

    shards = lax.axis_size(SEQ)
    prior = lax.ppermute(inputs[length - 8 :], SEQ, [(i, i + 1) for i in range(shards - 1)])
    starts = doc_start.reshape(8, HALF)
    main, lead = conv_main(counts, inputs, conv_weight, conv_bias, starts)
    own = conv_head(main, lead, prior)

    ct = lax.ppermute(own, ZL, [(TAU[i], i) for i in range(4)])
    f1 = around(own, X, 1)
    f3 = around(own, X, 3)
    f2 = around(own, X, 2)
    c1 = flipped(own, ZL)

    homes = lax.dynamic_index_in_dim(jnp.asarray(HOMES, jnp.int32), 4 * z + x, keepdims=False)
    where = jnp.concatenate([jnp.stack([x, z, core, count]).astype(jnp.int32), homes])
    keep, send = multiplied(False, where, own, f2, ct)
    got = flipped(send, CORE)
    first = encoded(False, where, keep, got)
    keep, send = multiplied(True, where, own, f2, f1, f3, ct, c1)
    coded = encoded(True, where, keep, flipped(send, CORE), first)
    quad, extra, message = decoded(lax.all_to_all(coded, CHIPS, split_axis=0, concat_axis=0, tiled=True))

    r2 = lax.ppermute(message, AXES, pairs[1])
    r1 = lax.ppermute(message, AXES, pairs[0])
    how = lax.dynamic_index_in_dim(jnp.asarray(table), lax.axis_index(AXES), keepdims=False)
    return assembled(how, quad, extra, r1, r2)


def solution(mesh):
    torus = Mesh(mesh.devices.reshape(SIZES), AXES)
    mp = (ZL, X)
    placed = (P(SEQ, mp), P(None, mp), P(mp), P(SEQ), P(SEQ))

    return jax.shard_map(on_device, mesh=torus, in_specs=placed, out_specs=P(SEQ, mp), check_vma=False)
```
